256 devices in a mesh: tile: 64 (over y, z, x_hi), band: 4 (over x_lo, core).
Axes of the slice: x: 4 (x_hi: 2, x_lo: 2; x = x_hi * 2 + x_lo), y: 4, z: 8, core: 2. Of those that a mesh axis runs over, the one named last changes fastest.
Arguments:
- background: float32 [36, 36, 64, 8, 128], P('band', None, 'tile'), may hold values from 0.2 to 2
- tangent: float32 [36, 36, 64, 8, 128], P('band', None, 'tile'), may hold values from -6 to 6
- sea_mask: int32 [64, 8, 128], P('tile'), may hold values 0 or 1
- coupling: float32 [36], P('band'), may hold values from 0.005 to 0.05
- freq_offsets: int32 [2], replicated, may hold values from 1 to 3, as said below
- dir_offsets: int32 [2], replicated, may hold values from 1 to 5
Outputs:
- background_out: float32 [36, 36, 64, 8, 128], P('band', None, 'tile')
- tangent_out: float32 [36, 36, 64, 8, 128], P('band', None, 'tile')
The draws below stay inside these ranges and needn't reach their ends.
Inputs may be any that keep to these rules, and one draw needn't show every extreme that they name: `freq_offsets`: one of the two offsets equals 3, the other is smaller.
All inputs are finite; a program needn't handle non-finite values. No bound on the sum of `sea_mask` on one device may be relied on, other than what follows from the above.
Results may differ from the reference program's by a relative error of at most 0.00002.
Values sent between devices are 32-bit elements; how exact they have to be, the bound alone decides.
A program may use at most 64 MiB of HBM per device.

```python
import math
import jax
import jax.numpy as jnp
from jax import lax

NF = 36
ND = 36
CLAT = 8
CLON = 128
TY = 4
FH = 3
STEPS = 2
SUBSTEPS = 2
TILES = 64


def draw_freq_offsets(key, part):
    first_key, second_key = jax.random.split(jax.random.fold_in(key, 11), 2)
    other = jax.random.randint(first_key, (), 1, FH)
    which = jax.random.randint(second_key, (), 0, 2)
    upper = jnp.where(which == 0, FH, other)
    lower = jnp.where(which == 0, other, FH)
    return jnp.stack([upper, lower]).astype(jnp.int32)


def plant(values, rng, least, high):
    extent = values.shape
    spot = [jax.random.randint(jax.random.fold_in(rng, axis), (), 0, extent[axis]) for axis in range(len(extent))]
    values = values.at[tuple(spot)].set(least)
    longest = extent.index(max(extent))
    spot[longest] = (spot[longest] + 1) % extent[longest]
    return values.at[tuple(spot)].set(high)


def block_scale(own_key, shape, pieces, low, largest):
    loudness = 1.0
    for position, blocks in pieces:
        heights = jax.random.uniform(jax.random.fold_in(jax.random.fold_in(own_key, 6), position), (blocks,), jnp.float32, low / len(pieces), largest / len(pieces))
        loudness = loudness * jnp.repeat(jnp.exp(heights), shape[position] // blocks).reshape((-1,) + (1,) * (len(shape) - 1 - position))
    return loudness


def gaussian(key, dims, deviation, bound, shards=(), kind=jnp.bfloat16):
    drawn = deviation * jax.random.normal(key, dims, jnp.float32)
    if shards:
        drawn = drawn * block_scale(key, dims, shards, -0.22, 0.18)
    return jnp.clip(drawn, -bound, bound).astype(kind)


def setup_inputs(seed: int = 0) -> dict:
    splits = jax.random.split(jax.random.key(seed), 7)
    background = jnp.clip(jnp.exp(math.log(2.0) - 2.3025851 * jax.random.uniform(splits[0], (NF, ND, TILES, CLAT, CLON), jnp.float32) ** block_scale(splits[0], (NF, ND, TILES, CLAT, CLON), ((0, 4), (2, 64)), -0.2, 0.2)), 0.2, 2.0)
    tangent = gaussian(splits[1], (NF, ND, TILES, CLAT, CLON), 1.0, 6.0, ((0, 4), (2, 64)), jnp.float32)
    sea_mask = plant((jax.random.randint(splits[2], (TILES, CLAT, CLON), 0, 5) < 4).astype(jnp.int32), jax.random.fold_in(splits[2], 1), 0, 1)
    coupling = jnp.clip(jnp.exp(math.log(0.05) - 2.3025851 * jax.random.uniform(splits[3], (NF,), jnp.float32) ** block_scale(splits[3], (NF,), ((0, 4),), -0.2, 0.2)), 0.005, 0.05)
    freq_offsets = draw_freq_offsets(jax.random.fold_in(splits[6], 71), 0)
    dir_offsets = jax.random.randint(splits[5], (2,), 1, 6).astype(jnp.int32)
    return dict(background=background, tangent=tangent, sea_mask=sea_mask, coupling=coupling, freq_offsets=freq_offsets, dir_offsets=dir_offsets)


weight_plus = 1.0 / 1.25 ** 4
weight_minus = 1.0 / 0.75 ** 4
weight_cross = 1.0 / (1.0 - 0.25 ** 2) ** 4
source_step = 0.5


def interaction(centre, tangent_c, upper_f, upper_t, lower_f, lower_t):
    linear = weight_plus * upper_f + weight_minus * lower_f
    rate = centre * centre * linear - weight_cross * centre * upper_f * lower_f
    change = (2.0 * centre * tangent_c * linear
              + centre * centre * (weight_plus * upper_t + weight_minus * lower_t)
              - weight_cross * (tangent_c * upper_f * lower_f + centre * upper_t * lower_f + centre * upper_f * lower_t))
    return rate, change


def apply_source(centre_pair, upper_pair, lower_pair, strength, dir_one, dir_two, dir_axis):
    upper_first = jnp.roll(upper_pair, -dir_one, dir_axis)
    lower_first = jnp.roll(lower_pair, dir_two, dir_axis)
    upper_second = jnp.roll(upper_pair, dir_one, dir_axis)
    lower_second = jnp.roll(lower_pair, -dir_two, dir_axis)
    rate_one, change_one = interaction(centre_pair[0], centre_pair[1], upper_first[0], upper_first[1], lower_first[0], lower_first[1])
    rate_two, change_two = interaction(centre_pair[0], centre_pair[1], upper_second[0], upper_second[1], lower_second[0], lower_second[1])
    background = centre_pair[0] - source_step * (strength * (rate_one + rate_two))
    tangent = centre_pair[1] - source_step * (strength * (change_one + change_two))
    return jnp.stack([background, tangent])


def upwind(padded, sea_float, rate_east, rate_west, rate_north, rate_south):
    centre = padded[..., 1:-1, 1:-1]
    west = padded[..., 1:-1, :-2]
    east = padded[..., 1:-1, 2:]
    south = padded[..., :-2, 1:-1]
    north = padded[..., 2:, 1:-1]
    return sea_float * (centre - rate_east * (centre - west) + rate_west * (east - centre)
                        - rate_north * (centre - south) + rate_south * (north - centre))


def to_grid(field, tiles_lon):
    field = jnp.roll(field, TY // 2, axis=-3)
    lead = field.shape[:-3]
    shaped = field.reshape(lead + (tiles_lon, TY, CLAT, CLON))
    count = len(lead)
    order = tuple(range(count)) + (count + 1, count + 2, count, count + 3)
    return shaped.transpose(order).reshape(lead + (TY * CLAT, tiles_lon * CLON))


def from_grid(grid, tiles_lon):
    lead = grid.shape[:-2]
    shaped = grid.reshape(lead + (TY, CLAT, tiles_lon, CLON))
    count = len(lead)
    order = tuple(range(count)) + (count + 2, count, count + 1, count + 3)
    tiles = shaped.transpose(order).reshape(lead + (TY * tiles_lon, CLAT, CLON))
    return jnp.roll(tiles, -(TY // 2), axis=-3)


def reference(background, tangent, sea_mask, coupling, freq_offsets, dir_offsets):
    tiles_lon = TILES // TY
    sea_float = sea_mask.astype(jnp.float32)
    sea_grid = to_grid(sea_float, tiles_lon)
    angles = (jnp.arange(ND, dtype=jnp.float32) + 0.5) * (2.0 * jnp.pi / ND)
    fields = jnp.stack([background, tangent], 1) * sea_float

    def propagate(level, field):
        speed = 0.7 * jnp.power(jnp.float32(1.1), -level.astype(jnp.float32))
        along_x = (speed * jnp.cos(angles))[:, None, None]
        along_y = (speed * jnp.sin(angles))[:, None, None]
        rate_east = jnp.maximum(along_x, 0.0)
        rate_west = jnp.maximum(-along_x, 0.0)
        rate_north = jnp.maximum(along_y, 0.0)
        rate_south = jnp.maximum(-along_y, 0.0)
        grid = to_grid(field, tiles_lon)
        for substep in range(SUBSTEPS):
            padded = jnp.pad(grid, ((0, 0), (0, 0), (1, 1), (0, 0)))
            padded = jnp.concatenate([padded[..., -1:], padded, padded[..., :1]], axis=-1)
            grid = upwind(padded, sea_grid, rate_east, rate_west, rate_north, rate_south)
        return from_grid(grid, tiles_lon)

    for model_step in range(STEPS):
        fields = lax.map(lambda item: propagate(item[0], item[1]), (jnp.arange(NF, dtype=jnp.int32), fields))
        padded = jnp.pad(fields, ((FH, FH), (0, 0), (0, 0), (0, 0), (0, 0), (0, 0)))

        def at_level(level):
            centre = lax.dynamic_index_in_dim(fields, level, 0, False)
            upper = lax.dynamic_index_in_dim(padded, FH + level + freq_offsets[0], 0, False)
            lower = lax.dynamic_index_in_dim(padded, FH + level - freq_offsets[1], 0, False)
            strength = lax.dynamic_index_in_dim(coupling, level, 0, False)
            return apply_source(centre, upper, lower, strength, dir_offsets[0], dir_offsets[1], 1)

        fields = lax.map(at_level, jnp.arange(NF, dtype=jnp.int32))
    return fields[:, 0], fields[:, 1]
```

```python
import math

import jax
import jax.numpy as jnp
from jax import lax
from jax.experimental import pallas as pl
from jax.experimental.pallas import tpu as pltpu
from jax.sharding import PartitionSpec as P

TY = 4
FH = 3
STEPS = 2
ND = 36
PAD = 5
WIDE = ND + 2 * PAD
HALF = ND // 2
GROUP = 3
MESH = pl.DeviceIdType.MESH

weight_plus = 1.0 / 1.25**4
weight_minus = 1.0 / 0.75**4
weight_cross = 1.0 / (1.0 - 0.25**2) ** 4
source_step = 0.5

COS = [math.cos((j + 0.5) * 2.0 * math.pi / ND) for j in range(ND)]
SIN = [math.sin((j + 0.5) * 2.0 * math.pi / ND) for j in range(ND)]
EASTWARD = [j for j in range(ND) if COS[j] > 0]
WESTWARD = [j for j in range(ND) if COS[j] < 0]
NORTHWARD = [j for j in range(ND) if SIN[j] > 0]
SOUTHWARD = [j for j in range(ND) if SIN[j] < 0]


def kernel(
    n_k,
    back_in,
    tang_in,
    mask_in,
    coupling,
    freq_off,
    dir_off,
    back_out,
    tang_out,
    state,
    low_ext_0,
    low_ext_1,
    high_ext_0,
    high_ext_1,
    row_send,
    row_recv,
    col_send,
    col_recv,
    speed,
    row_ssem,
    row_rsem,
    col_ssem,
    col_rsem,
    band_ssem,
    band_rsem,
):
    tiles = lax.axis_size("tile")
    bands = lax.axis_size("band")
    tile = lax.axis_index("tile")
    band = lax.axis_index("band")
    lat = lax.rem(tile + TY // 2, TY)
    north = lax.rem(tile + 1, tiles)
    south = lax.rem(tile + tiles - 1, tiles)
    east = lax.rem(tile + TY, tiles)
    west = lax.rem(tile + tiles - TY, tiles)
    has_north = lat < TY - 1
    has_south = lat > 0
    has_up = band < bands - 1
    has_down = band > 0
    groups = n_k // GROUP
    low_exts = (low_ext_0, low_ext_1)
    high_exts = (high_ext_0, high_ext_1)
    inputs = (back_in, tang_in)
    outputs = (back_out, tang_out)

    def row_copy(slot, side, g):
        ks = pl.ds(g * GROUP, GROUP)
        return pltpu.make_async_remote_copy(
            src_ref=row_send.at[slot, side, ks],
            dst_ref=row_recv.at[slot, side, ks],
            send_sem=row_ssem.at[slot, side, g],
            recv_sem=row_rsem.at[slot, side, g],
            device_id={"tile": north if side == 0 else south},
            device_id_type=MESH,
        )

    def col_copy(slot, side, g):
        return pltpu.make_async_remote_copy(
            src_ref=col_send.at[slot, side, g],
            dst_ref=col_recv.at[slot, side, g],
            send_sem=col_ssem.at[slot, side, g],
            recv_sem=col_rsem.at[slot, side, g],
            device_id={"tile": east if side == 0 else west},
            device_id_type=MESH,
        )

    def band_copy(step, side):
        if side == 0:
            src = state.at[step, :, pl.ds(n_k - FH, FH), pl.ds(PAD, ND)]
            dst = low_exts[step].at[:, pl.ds(0, FH), pl.ds(PAD, ND)]
            target = lax.rem(band + 1, bands)
        else:
            src = state.at[step, :, pl.ds(0, FH), pl.ds(PAD, ND)]
            dst = high_exts[step].at[:, pl.ds(FH - 1, FH), pl.ds(PAD, ND)]
            target = lax.rem(band + bands - 1, bands)
        return pltpu.make_async_remote_copy(
            src_ref=src,
            dst_ref=dst,
            send_sem=band_ssem.at[step, side],
            recv_sem=band_rsem.at[step, side],
            device_id={"band": target},
            device_id_type=MESH,
        )

    def send_halo(slot, g):
        @pl.when(has_north)
        def _():
            row_copy(slot, 0, g).start()

        @pl.when(has_south)
        def _():
            row_copy(slot, 1, g).start()

        col_copy(slot, 0, g).start()
        col_copy(slot, 1, g).start()

    def wait_halo(slot, g):
        @pl.when(has_south)
        def _():
            row_copy(slot, 0, g).wait_recv()

        @pl.when(has_north)
        def _():
            row_copy(slot, 1, g).wait_recv()

        col_copy(slot, 0, g).wait_recv()
        col_copy(slot, 1, g).wait_recv()

    barrier = pltpu.get_barrier_semaphore()
    for cond, target in (
        (None, {"tile": east}),
        (None, {"tile": west}),
        (has_north, {"tile": north}),
        (has_south, {"tile": south}),
        (has_up, {"band": lax.rem(band + 1, bands)}),
        (has_down, {"band": lax.rem(band + bands - 1, bands)}),
    ):

        def greet(target=target):
            pl.semaphore_signal(barrier, inc=1, device_id=target, device_id_type=MESH)

        if cond is None:
            greet()
        else:
            pl.when(cond)(greet)

    base = jnp.float32(0.7)
    for b in range(1, 4):
        base = jnp.where(band == b, jnp.float32(0.7 * 1.1 ** (-n_k * b)), base)
    for k in range(n_k):
        speed[k] = base * jnp.float32(1.1 ** (-k))

    lane = lax.broadcasted_iota(jnp.int32, (8, 128), 1)
    sub = lax.broadcasted_iota(jnp.int32, (8, 128), 0)
    mask = mask_in[0].astype(jnp.float32)
    zeros = jnp.zeros((8, 128), jnp.float32)

    def zero_rows(side):
        def slots(i, _):
            row_recv[i // n_k, side, lax.rem(i, n_k)] = jnp.zeros((ND, 128), jnp.float32)
            return 0

        lax.fori_loop(0, 2 * STEPS * n_k, slots, 0)

    pl.when(jnp.logical_not(has_south))(lambda: zero_rows(0))
    pl.when(jnp.logical_not(has_north))(lambda: zero_rows(1))

    def zero_ext(ext, first):
        def rows(r, _):
            ext[r // FH, first + lax.rem(r, FH)] = jnp.zeros((WIDE, 8, 128), jnp.float32)
            return 0

        lax.fori_loop(0, 2 * FH, rows, 0)

    for step in range(STEPS):
        pl.when(jnp.logical_not(has_down))(lambda: zero_ext(low_exts[step], 0))
        pl.when(jnp.logical_not(has_up))(lambda: zero_ext(high_exts[step], FH - 1))

    def pack_bin(slot, f, k, j, new, parts):
        r = f * HALF + (j if SIN[j] > 0 else j - HALF)
        if SIN[j] > 0:
            row_send[slot, 0, k, pl.ds(r, 1), :] = new[7:8, :]
        else:
            row_send[slot, 1, k, pl.ds(r, 1), :] = new[0:1, :]
        if COS[j] > 0:
            c = f * HALF + EASTWARD.index(j)
            moved = pltpu.roll(new, (c + 1) % 128, 1)
            return [jnp.where(lane == c, moved, parts[0]), parts[1]]
        c = f * HALF + WESTWARD.index(j)
        moved = new if c == 0 else pltpu.roll(new, c, 1)
        return [parts[0], jnp.where(lane == c, moved, parts[1])]

    def join(sums, parts, i):
        return tuple(s + pltpu.roll(p, i * ND, 1) for s, p in zip(sums, parts))

    def finish_pack(slot, g, sums):
        col_send[slot, 0, g] = sums[0]
        col_send[slot, 1, g] = sums[1]

    def write_state(step, f, k, j, new):
        state[step, f, k, PAD + j] = new
        if j >= ND - PAD:
            state[step, f, k, j - (ND - PAD)] = new
        if j < PAD:
            state[step, f, k, PAD + ND + j] = new

    def entry(i, _):
        g = lax.rem(2 * i, groups)

        def at_level(kk, sums):
            k = g * GROUP + kk
            parts = [zeros, zeros]
            for f in range(2):
                for j in range(ND):
                    new = inputs[f][k, j, 0] * mask
                    state[0, f, k, PAD + j] = new
                    parts = pack_bin(0, f, k, j, new, parts)
            return join(sums, parts, kk)

        finish_pack(0, g, lax.fori_loop(0, GROUP, at_level, (zeros, zeros)))
        return 0

    lax.fori_loop(0, groups, entry, 0)

    peers = (
        2
        + has_north.astype(jnp.int32)
        + has_south.astype(jnp.int32)
        + has_up.astype(jnp.int32)
        + has_down.astype(jnp.int32)
    )
    pl.semaphore_wait(barrier, peers)

    for g in (0, 2, 1):
        send_halo(0, g)

    def substep(step, part):
        slot = 2 * step + part

        def group(i, _):
            g = lax.rem(2 * i + step, groups)
            wait_halo(slot, g)
            col_low = col_recv[slot, 0, g]
            col_high = col_recv[slot, 1, g]

            def at_level(kk, sums):
                k = g * GROUP + kk
                rate = speed[k]
                back = lax.rem(128 - kk * ND, 128)
                halo_w = pltpu.roll(col_low, back, 1)
                halo_e = pltpu.roll(col_high, back, 1)
                parts = [zeros, zeros]
                for j in range(ND):
                    rate_x = rate * jnp.float32(abs(COS[j]))
                    rate_y = rate * jnp.float32(abs(SIN[j]))
                    rate_0 = jnp.float32(1.0) - rate_x - rate_y
                    for f in range(2):
                        old = state[step, f, k, PAD + j]
                        if COS[j] > 0:
                            c = f * HALF + EASTWARD.index(j)
                            edge = halo_w if c == 0 else pltpu.roll(halo_w, 128 - c, 1)
                            side = jnp.where(lane == 0, edge, pltpu.roll(old, 1, 1))
                        else:
                            c = f * HALF + WESTWARD.index(j)
                            edge = pltpu.roll(halo_e, 127 - c, 1)
                            side = jnp.where(lane == 127, edge, pltpu.roll(old, 127, 1))
                        r = f * HALF + (j if SIN[j] > 0 else j - HALF)
                        if SIN[j] > 0:
                            row = row_recv[slot, 0, k, pl.ds(r, 1), :]
                            above = jnp.where(sub == 0, row, pltpu.roll(old, 1, 0))
                        else:
                            row = row_recv[slot, 1, k, pl.ds(r, 1), :]
                            above = jnp.where(sub == 7, row, pltpu.roll(old, 7, 0))
                        new = mask * (rate_0 * old + rate_x * side + rate_y * above)
                        if part == 0:
                            state[step, f, k, PAD + j] = new
                            parts = pack_bin(slot + 1, f, k, j, new, parts)
                        else:
                            write_state(step, f, k, j, new)
                if part == 0:
                    return join(sums, parts, kk)
                return sums

            sums = lax.fori_loop(0, GROUP, at_level, (zeros, zeros))
            if part == 0:
                finish_pack(slot + 1, g, sums)
                send_halo(slot + 1, g)
            else:

                @pl.when(jnp.logical_and(g == 0, has_down))
                def _():
                    band_copy(step, 1).start()

                @pl.when(jnp.logical_and(g == groups - 1, has_up))
                def _():
                    band_copy(step, 0).start()

            return 0

        lax.fori_loop(0, groups, group, 0)

    def wrap(ext, first):
        def one(i, _):
            f, k = i // FH, first + lax.rem(i, FH)
            ext[f, k, pl.ds(0, PAD)] = ext[f, k, pl.ds(ND, PAD)]
            ext[f, k, pl.ds(ND + PAD, PAD)] = ext[f, k, pl.ds(PAD, PAD)]
            return 0

        lax.fori_loop(0, 2 * FH, one, 0)

    def lend(ext, step, first, k0):
        def one(i, _):
            f, k = i // (FH - 1), lax.rem(i, FH - 1)
            ext[f, first + k] = state[step, f, k0 + k]
            return 0

        lax.fori_loop(0, 2 * (FH - 1), one, 0)

    def source(step, g, upper, lower):
        up = jnp.maximum(freq_off[0], 1)
        down = jnp.maximum(freq_off[1], 1)
        e = dir_off[0]
        h = dir_off[1]
        slot = 2 * step + 2

        def at_level(kk, sums):
            k = g * GROUP + kk
            strength = source_step * coupling[k]
            parts = [zeros, zeros]
            for j in range(ND):
                f0 = state[step, 0, k, PAD + j]
                g0 = state[step, 1, k, PAD + j]
                fp1, gp1 = upper(k + up, j + e)
                fm1, gm1 = lower(k - down, j - h)
                fp2, gp2 = upper(k + up, j - e)
                fm2, gm2 = lower(k - down, j + h)
                linear = weight_plus * (fp1 + fp2) + weight_minus * (fm1 + fm2)
                linear_t = weight_plus * (gp1 + gp2) + weight_minus * (gm1 + gm2)
                cross = weight_cross * (fp1 * fm1 + fp2 * fm2)
                cross_t = weight_cross * (gp1 * fm1 + fp1 * gm1 + gp2 * fm2 + fp2 * gm2)
                lead = f0 * linear
                rest = lead - cross
                rate = f0 * rest
                change = g0 * (lead + rest) + f0 * (f0 * linear_t - cross_t)
                for f, new in ((0, f0 - strength * rate), (1, g0 - strength * change)):
                    if step < STEPS - 1:
                        state[step + 1, f, k, PAD + j] = new
                        parts = pack_bin(slot, f, k, j, new, parts)
                    else:
                        outputs[f][k, j, 0] = new
            return join(sums, parts, kk) if step < STEPS - 1 else sums

        sums = lax.fori_loop(0, GROUP, at_level, (zeros, zeros))
        if step < STEPS - 1:
            finish_pack(slot, g, sums)
            send_halo(slot, g)

    def model_step(step):
        low_ext, high_ext = low_exts[step], high_exts[step]
        substep(step, 0)
        substep(step, 1)

        def local(k, j):
            return state[step, 0, k, PAD + j], state[step, 1, k, PAD + j]

        def low(k, j):
            return low_ext[0, k + FH, PAD + j], low_ext[1, k + FH, PAD + j]

        def high(k, j):
            i = k - (n_k - FH + 1)
            return high_ext[0, i, PAD + j], high_ext[1, i, PAD + j]

        source(step, 1, local, local)
        lend(low_ext, step, FH, 0)
        lend(high_ext, step, 0, n_k - FH + 1)

        @pl.when(has_down)
        def _():
            band_copy(step, 0).wait_recv()
            wrap(low_ext, 0)

        source(step, 0, local, low)

        @pl.when(has_up)
        def _():
            band_copy(step, 1).wait_recv()
            wrap(high_ext, FH - 1)

        source(step, groups - 1, high, local)

    for step in range(STEPS):
        model_step(step)

    def drain(i, _):
        slot, g = i // groups, lax.rem(i, groups)

        @pl.when(has_north)
        def _():
            row_copy(slot, 0, g).wait_send()

        @pl.when(has_south)
        def _():
            row_copy(slot, 1, g).wait_send()

        col_copy(slot, 0, g).wait_send()
        col_copy(slot, 1, g).wait_send()
        return 0

    lax.fori_loop(0, 2 * STEPS * groups, drain, 0)
    for step in range(STEPS):

        @pl.when(has_up)
        def _():
            band_copy(step, 0).wait_send()

        @pl.when(has_down)
        def _():
            band_copy(step, 1).wait_send()


def body(background, tangent, sea_mask, coupling, freq_offsets, dir_offsets):
    n_k = background.shape[0]
    groups = n_k // GROUP
    slots = 2 * STEPS
    f32 = jnp.float32
    dma = pltpu.SemaphoreType.DMA
    out = jax.ShapeDtypeStruct(background.shape, f32)
    return pl.pallas_call(
        lambda *refs: kernel(n_k, *refs),
        out_shape=(out, out),
        in_specs=[
            pl.BlockSpec(memory_space=pltpu.VMEM),
            pl.BlockSpec(memory_space=pltpu.VMEM),
            pl.BlockSpec(memory_space=pltpu.VMEM),
            pl.BlockSpec(memory_space=pltpu.SMEM),
            pl.BlockSpec(memory_space=pltpu.SMEM),
            pl.BlockSpec(memory_space=pltpu.SMEM),
        ],
        out_specs=(pl.BlockSpec(memory_space=pltpu.VMEM), pl.BlockSpec(memory_space=pltpu.VMEM)),
        scratch_shapes=[
            pltpu.VMEM((STEPS, 2, n_k, WIDE, 8, 128), f32),
            pltpu.VMEM((2, 2 * FH - 1, WIDE, 8, 128), f32),
            pltpu.VMEM((2, 2 * FH - 1, WIDE, 8, 128), f32),
            pltpu.VMEM((2, 2 * FH - 1, WIDE, 8, 128), f32),
            pltpu.VMEM((2, 2 * FH - 1, WIDE, 8, 128), f32),
            pltpu.VMEM((slots, 2, n_k, ND, 128), f32),
            pltpu.VMEM((slots, 2, n_k, ND, 128), f32),
            pltpu.VMEM((slots, 2, groups, 8, 128), f32),
            pltpu.VMEM((slots, 2, groups, 8, 128), f32),
            pltpu.SMEM((n_k,), f32),
            dma((slots, 2, groups)),
            dma((slots, 2, groups)),
            dma((slots, 2, groups)),
            dma((slots, 2, groups)),
            dma((STEPS, 2)),
            dma((STEPS, 2)),
        ],
        compiler_params=pltpu.CompilerParams(
            collective_id=0, has_side_effects=True, vmem_limit_bytes=48 * 1024 * 1024
        ),
        name="wave_steps",
    )(background, tangent, sea_mask, coupling, freq_offsets, dir_offsets)


def solution(mesh):
    in_specs = (
        P("band", None, "tile", None, None),
        P("band", None, "tile", None, None),
        P("tile", None, None),
        P("band"),
        P(),
        P(),
    )
    out_specs = (P("band", None, "tile", None, None), P("band", None, "tile", None, None))
    return jax.shard_map(body, mesh=mesh, in_specs=in_specs, out_specs=out_specs, check_vma=False)
```

```python
import math

import jax
import jax.numpy as jnp
from jax import lax
from jax.experimental import pallas as pl
from jax.experimental.pallas import tpu as pltpu
from jax.sharding import PartitionSpec as P

TY = 4
FH = 3
STEPS = 2
ND = 36
PAD = 5
WIDE = ND + 2 * PAD
HALF = ND // 2
GROUP = 3
MESH = pl.DeviceIdType.MESH

weight_plus = 1.0 / 1.25**4
weight_minus = 1.0 / 0.75**4
weight_cross = 1.0 / (1.0 - 0.25**2) ** 4
source_step = 0.5

COS = [math.cos((j + 0.5) * 2.0 * math.pi / ND) for j in range(ND)]
SIN = [math.sin((j + 0.5) * 2.0 * math.pi / ND) for j in range(ND)]
EASTWARD = [j for j in range(ND) if COS[j] > 0]
WESTWARD = [j for j in range(ND) if COS[j] < 0]
NORTHWARD = [j for j in range(ND) if SIN[j] > 0]
SOUTHWARD = [j for j in range(ND) if SIN[j] < 0]


def kernel(
    n_k,
    back_in,
    tang_in,
    mask_hbm,
    coupling_hbm,
    freq_hbm,
    dir_hbm,
    back_out,
    tang_out,
    state_0,
    state_1,
    low_ext_0,
    low_ext_1,
    high_ext_0,
    high_ext_1,
    row_send,
    row_recv,
    col_send,
    col_recv,
    mask_in,
    coupling,
    freq_off,
    dir_off,
    speed,
    result,
    load_sem,
    store_sem,
    small_sem,
    row_ssem,
    row_rsem,
    col_ssem,
    col_rsem,
    band_ssem,
    band_rsem,
):
    tiles = lax.axis_size("tile")
    bands = lax.axis_size("band")
    tile = lax.axis_index("tile")
    band = lax.axis_index("band")
    lat = lax.rem(tile + TY // 2, TY)
    north = lax.rem(tile + 1, tiles)
    south = lax.rem(tile + tiles - 1, tiles)
    east = lax.rem(tile + TY, tiles)
    west = lax.rem(tile + tiles - TY, tiles)
    has_north = lat < TY - 1
    has_south = lat > 0
    has_up = band < bands - 1
    has_down = band > 0
    groups = n_k // GROUP
    states = (state_0, state_1)
    low_exts = (low_ext_0, low_ext_1)
    high_exts = (high_ext_0, high_ext_1)
    inputs = (back_in, tang_in)
    outputs = (back_out, tang_out)

    def load_copy(f, g):
        return pltpu.make_async_copy(
            inputs[f].at[pl.ds(g * GROUP, GROUP), :, 0],
            state_0.at[f, pl.ds(g * GROUP, GROUP), pl.ds(PAD, ND)],
            load_sem.at[f, g],
        )

    def store_copy(f, g):
        return pltpu.make_async_copy(
            result.at[f, pl.ds(g * GROUP, GROUP)],
            outputs[f].at[pl.ds(g * GROUP, GROUP), :, 0],
            store_sem.at[f, g],
        )

    small = [
        pltpu.make_async_copy(src, dst, small_sem.at[i])
        for i, (src, dst) in enumerate(
            (
                (mask_hbm, mask_in),
                (coupling_hbm, coupling),
                (freq_hbm, freq_off),
                (dir_hbm, dir_off),
            )
        )
    ]

    def row_copy(slot, side, g):
        ks = pl.ds(g * GROUP, GROUP)
        return pltpu.make_async_remote_copy(
            src_ref=row_send.at[slot, side, ks],
            dst_ref=row_recv.at[slot, side, ks],
            send_sem=row_ssem.at[slot, side, g],
            recv_sem=row_rsem.at[slot, side, g],
            device_id={"tile": north if side == 0 else south},
            device_id_type=MESH,
        )

    def col_copy(slot, side, g):
        return pltpu.make_async_remote_copy(
            src_ref=col_send.at[slot, side, g],
            dst_ref=col_recv.at[slot, side, g],
            send_sem=col_ssem.at[slot, side, g],
            recv_sem=col_rsem.at[slot, side, g],
            device_id={"tile": east if side == 0 else west},
            device_id_type=MESH,
        )

    def band_copy(step, side):
        if side == 0:
            src = states[step].at[:, pl.ds(n_k - FH, FH), pl.ds(PAD, ND)]
            dst = low_exts[step].at[:, pl.ds(0, FH), pl.ds(PAD, ND)]
            target = lax.rem(band + 1, bands)
        else:
            src = states[step].at[:, pl.ds(0, FH), pl.ds(PAD, ND)]
            dst = high_exts[step].at[:, pl.ds(FH - 1, FH), pl.ds(PAD, ND)]
            target = lax.rem(band + bands - 1, bands)
        return pltpu.make_async_remote_copy(
            src_ref=src,
            dst_ref=dst,
            send_sem=band_ssem.at[step, side],
            recv_sem=band_rsem.at[step, side],
            device_id={"band": target},
            device_id_type=MESH,
        )

    def send_halo(slot, g):
        @pl.when(has_north)
        def _():
            row_copy(slot, 0, g).start()

        @pl.when(has_south)
        def _():
            row_copy(slot, 1, g).start()

        col_copy(slot, 0, g).start()
        col_copy(slot, 1, g).start()

    def wait_halo(slot, g):
        @pl.when(has_south)
        def _():
            row_copy(slot, 0, g).wait_recv()

        @pl.when(has_north)
        def _():
            row_copy(slot, 1, g).wait_recv()

        col_copy(slot, 0, g).wait_recv()
        col_copy(slot, 1, g).wait_recv()

    for copy in small:
        copy.start()
    for g in (0, 2, 1):
        for f in range(2):
            load_copy(f, g).start()

    barrier = pltpu.get_barrier_semaphore()
    for cond, target in (
        (None, {"tile": east}),
        (None, {"tile": west}),
        (has_north, {"tile": north}),
        (has_south, {"tile": south}),
        (has_up, {"band": lax.rem(band + 1, bands)}),
        (has_down, {"band": lax.rem(band + bands - 1, bands)}),
    ):

        def greet(target=target):
            pl.semaphore_signal(barrier, inc=1, device_id=target, device_id_type=MESH)

        if cond is None:
            greet()
        else:
            pl.when(cond)(greet)

    base = jnp.float32(0.7)
    for b in range(1, 4):
        base = jnp.where(band == b, jnp.float32(0.7 * 1.1 ** (-n_k * b)), base)
    for k in range(n_k):
        speed[k] = base * jnp.float32(1.1 ** (-k))

    lane = lax.broadcasted_iota(jnp.int32, (8, 128), 1)
    sub = lax.broadcasted_iota(jnp.int32, (8, 128), 0)
    for copy in small:
        copy.wait()
    mask = mask_in[0].astype(jnp.float32)
    zeros = jnp.zeros((8, 128), jnp.float32)

    def zero_rows(side):
        def slots(i, _):
            row_recv[i // n_k, side, lax.rem(i, n_k)] = jnp.zeros((2, HALF, 128), jnp.float32)
            return 0

        lax.fori_loop(0, 2 * STEPS * n_k, slots, 0)

    pl.when(jnp.logical_not(has_south))(lambda: zero_rows(0))
    pl.when(jnp.logical_not(has_north))(lambda: zero_rows(1))

    def zero_ext(ext, first):
        def rows(r, _):
            ext[r // FH, first + lax.rem(r, FH)] = jnp.zeros((WIDE, 8, 128), jnp.float32)
            return 0

        lax.fori_loop(0, 2 * FH, rows, 0)

    for step in range(STEPS):
        pl.when(jnp.logical_not(has_down))(lambda: zero_ext(low_exts[step], 0))
        pl.when(jnp.logical_not(has_up))(lambda: zero_ext(high_exts[step], FH - 1))

    def pack_bin(f, kk, j, new, parts):
        if COS[j] > 0:
            c = kk * ND + f * HALF + EASTWARD.index(j)
            moved = pltpu.roll(new, (c + 1) % 128, 1)
            return [jnp.where(lane == c, moved, parts[0]), parts[1]]
        c = kk * ND + f * HALF + WESTWARD.index(j)
        moved = new if c == 0 else pltpu.roll(new, c, 1)
        return [parts[0], jnp.where(lane == c, moved, parts[1])]

    def finish_pack(state, slot, g, parts):
        rows = state.reshape(2, n_k, WIDE * 8, 128)
        for kk in range(GROUP):
            k = g * GROUP + kk
            for f in range(2):
                row_send[slot, 0, k, f] = rows[f, k, pl.ds(8 * PAD + 7, HALF, stride=8), :]
                row_send[slot, 1, k, f] = rows[f, k, pl.ds(8 * (PAD + HALF), HALF, stride=8), :]
        col_send[slot, 0, g] = parts[0]
        col_send[slot, 1, g] = parts[1]

    def write_state(step, f, k, j, new):
        state = states[step]
        state[f, k, PAD + j] = new
        if j >= ND - PAD:
            state[f, k, j - (ND - PAD)] = new
        if j < PAD:
            state[f, k, PAD + ND + j] = new

    def entry(i, _):
        g = lax.rem(2 * i, groups)

        for f in range(2):
            load_copy(f, g).wait()
        parts = [zeros, zeros]
        for kk in range(GROUP):
            k = g * GROUP + kk
            for f in range(2):
                for j in range(ND):
                    new = state_0[f, k, PAD + j] * mask
                    state_0[f, k, PAD + j] = new
                    parts = pack_bin(f, kk, j, new, parts)
        finish_pack(state_0, 0, g, parts)
        return 0

    lax.fori_loop(0, groups, entry, 0)

    peers = (
        2
        + has_north.astype(jnp.int32)
        + has_south.astype(jnp.int32)
        + has_up.astype(jnp.int32)
        + has_down.astype(jnp.int32)
    )
    pl.semaphore_wait(barrier, peers)

    for g in (0, 2, 1):
        send_halo(0, g)

    def substep(step, part):
        slot = 2 * step + part

        def group(i, _):
            g = lax.rem(2 * i + step, groups)
            wait_halo(slot, g)
            col_low = col_recv[slot, 0, g]
            col_high = col_recv[slot, 1, g]

            for kk in range(GROUP):
                k = g * GROUP + kk
                rate = speed[k]
                for j in range(ND):
                    rate_x = rate * jnp.float32(abs(COS[j]))
                    rate_y = rate * jnp.float32(abs(SIN[j]))
                    rate_0 = jnp.float32(1.0) - rate_x - rate_y
                    for f in range(2):
                        old = states[step][f, k, PAD + j]
                        if COS[j] > 0:
                            c = kk * ND + f * HALF + EASTWARD.index(j)
                            edge = col_low if c == 0 else pltpu.roll(col_low, 128 - c, 1)
                            side = jnp.where(lane == 0, edge, pltpu.roll(old, 1, 1))
                        else:
                            c = kk * ND + f * HALF + WESTWARD.index(j)
                            edge = pltpu.roll(col_high, 127 - c, 1)
                            side = jnp.where(lane == 127, edge, pltpu.roll(old, 127, 1))
                        r = j if SIN[j] > 0 else j - HALF
                        if SIN[j] > 0:
                            row = row_recv[slot, 0, k, f, pl.ds(r, 1), :]
                            above = jnp.where(sub == 0, row, pltpu.roll(old, 1, 0))
                        else:
                            row = row_recv[slot, 1, k, f, pl.ds(r, 1), :]
                            above = jnp.where(sub == 7, row, pltpu.roll(old, 7, 0))
                        new = mask * (rate_0 * old + rate_x * side + rate_y * above)
                        if part == 0:
                            states[step][f, k, PAD + j] = new
                        else:
                            write_state(step, f, k, j, new)
            if part == 0:

                @pl.when(g >= 0)
                def _():
                    parts = [zeros, zeros]
                    for kk in range(GROUP):
                        k = g * GROUP + kk
                        for f in range(2):
                            for j in range(ND):
                                parts = pack_bin(f, kk, j, states[step][f, k, PAD + j], parts)
                    finish_pack(states[step], slot + 1, g, parts)

                send_halo(slot + 1, g)
            else:

                @pl.when(jnp.logical_and(g == 0, has_down))
                def _():
                    band_copy(step, 1).start()

                @pl.when(jnp.logical_and(g == groups - 1, has_up))
                def _():
                    band_copy(step, 0).start()

            return 0

        lax.fori_loop(0, groups, group, 0)

    def wrap(ext, first):
        def one(i, _):
            f, k = i // FH, first + lax.rem(i, FH)
            ext[f, k, pl.ds(0, PAD)] = ext[f, k, pl.ds(ND, PAD)]
            ext[f, k, pl.ds(ND + PAD, PAD)] = ext[f, k, pl.ds(PAD, PAD)]
            return 0

        lax.fori_loop(0, 2 * FH, one, 0)

    def lend(ext, step, first, k0):
        def one(i, _):
            f, k = i // (FH - 1), lax.rem(i, FH - 1)
            ext[f, first + k] = states[step][f, k0 + k]
            return 0

        lax.fori_loop(0, 2 * (FH - 1), one, 0)

    def source(step, g, upper, lower):
        up = jnp.maximum(freq_off[0], 1)
        down = jnp.maximum(freq_off[1], 1)
        e = dir_off[0]
        h = dir_off[1]
        slot = 2 * step + 2

        parts = [zeros, zeros]
        for kk in range(GROUP):
            k = g * GROUP + kk
            strength = source_step * coupling[k]
            for j in range(ND):
                f0 = states[step][0, k, PAD + j]
                g0 = states[step][1, k, PAD + j]
                fp1, gp1 = upper(k + up, j + e)
                fm1, gm1 = lower(k - down, j - h)
                fp2, gp2 = upper(k + up, j - e)
                fm2, gm2 = lower(k - down, j + h)
                linear = weight_plus * (fp1 + fp2) + weight_minus * (fm1 + fm2)
                linear_t = weight_plus * (gp1 + gp2) + weight_minus * (gm1 + gm2)
                cross = weight_cross * (fp1 * fm1 + fp2 * fm2)
                cross_t = weight_cross * (gp1 * fm1 + fp1 * gm1 + gp2 * fm2 + fp2 * gm2)
                lead = f0 * linear
                rest = lead - cross
                rate = f0 * rest
                change = g0 * (lead + rest) + f0 * (f0 * linear_t - cross_t)
                for f, new in ((0, f0 - strength * rate), (1, g0 - strength * change)):
                    if step < STEPS - 1:
                        states[step + 1][f, k, PAD + j] = new
                        parts = pack_bin(f, kk, j, new, parts)
                    else:
                        result[f, k, j] = new
        if step < STEPS - 1:
            finish_pack(states[step + 1], slot, g, parts)
            send_halo(slot, g)
        else:
            for f in range(2):
                store_copy(f, g).start()

    def model_step(step):
        low_ext, high_ext = low_exts[step], high_exts[step]
        substep(step, 0)
        substep(step, 1)

        def local(k, j):
            return states[step][0, k, PAD + j], states[step][1, k, PAD + j]

        def low(k, j):
            return low_ext[0, k + FH, PAD + j], low_ext[1, k + FH, PAD + j]

        def high(k, j):
            i = k - (n_k - FH + 1)
            return high_ext[0, i, PAD + j], high_ext[1, i, PAD + j]

        source(step, 1, local, local)
        lend(low_ext, step, FH, 0)
        lend(high_ext, step, 0, n_k - FH + 1)

        @pl.when(has_down)
        def _():
            band_copy(step, 0).wait_recv()
            wrap(low_ext, 0)

        source(step, 0, local, low)

        @pl.when(has_up)
        def _():
            band_copy(step, 1).wait_recv()
            wrap(high_ext, FH - 1)

        source(step, groups - 1, high, local)

    for step in range(STEPS):
        model_step(step)

    for g in range(groups):
        for f in range(2):
            store_copy(f, g).wait()

    def drain(i, _):
        slot, g = i // groups, lax.rem(i, groups)

        @pl.when(has_north)
        def _():
            row_copy(slot, 0, g).wait_send()

        @pl.when(has_south)
        def _():
            row_copy(slot, 1, g).wait_send()

        col_copy(slot, 0, g).wait_send()
        col_copy(slot, 1, g).wait_send()
        return 0

    lax.fori_loop(0, 2 * STEPS * groups, drain, 0)
    for step in range(STEPS):

        @pl.when(has_up)
        def _():
            band_copy(step, 0).wait_send()

        @pl.when(has_down)
        def _():
            band_copy(step, 1).wait_send()


def body(background, tangent, sea_mask, coupling, freq_offsets, dir_offsets):
    n_k = background.shape[0]
    groups = n_k // GROUP
    slots = 2 * STEPS
    f32 = jnp.float32
    dma = pltpu.SemaphoreType.DMA
    out = jax.ShapeDtypeStruct(background.shape, f32)
    return pl.pallas_call(
        lambda *refs: kernel(n_k, *refs),
        out_shape=(out, out),
        in_specs=[pl.BlockSpec(memory_space=pltpu.HBM)] * 6,
        out_specs=(pl.BlockSpec(memory_space=pl.ANY), pl.BlockSpec(memory_space=pl.ANY)),
        scratch_shapes=[
            pltpu.VMEM((2, n_k, WIDE, 8, 128), f32),
            pltpu.VMEM((2, n_k, WIDE, 8, 128), f32),
            pltpu.VMEM((2, 2 * FH - 1, WIDE, 8, 128), f32),
            pltpu.VMEM((2, 2 * FH - 1, WIDE, 8, 128), f32),
            pltpu.VMEM((2, 2 * FH - 1, WIDE, 8, 128), f32),
            pltpu.VMEM((2, 2 * FH - 1, WIDE, 8, 128), f32),
            pltpu.VMEM((slots, 2, n_k, 2, HALF, 128), f32),
            pltpu.VMEM((slots, 2, n_k, 2, HALF, 128), f32),
            pltpu.VMEM((slots, 2, groups, 8, 128), f32),
            pltpu.VMEM((slots, 2, groups, 8, 128), f32),
            pltpu.VMEM((1, 8, 128), jnp.int32),
            pltpu.SMEM((n_k,), f32),
            pltpu.SMEM((2,), jnp.int32),
            pltpu.SMEM((2,), jnp.int32),
            pltpu.SMEM((n_k,), f32),
            pltpu.VMEM((2, n_k, ND, 8, 128), f32),
            dma((2, groups)),
            dma((2, groups)),
            dma((4,)),
            dma((slots, 2, groups)),
            dma((slots, 2, groups)),
            dma((slots, 2, groups)),
            dma((slots, 2, groups)),
            dma((STEPS, 2)),
            dma((STEPS, 2)),
        ],
        compiler_params=pltpu.CompilerParams(
            collective_id=0, has_side_effects=True, vmem_limit_bytes=67043328
        ),
        name="wave_steps",
    )(background, tangent, sea_mask, coupling, freq_offsets, dir_offsets)


def solution(mesh):
    in_specs = (
        P("band", None, "tile", None, None),
        P("band", None, "tile", None, None),
        P("tile", None, None),
        P("band"),
        P(),
        P(),
    )
    out_specs = (P("band", None, "tile", None, None), P("band", None, "tile", None, None))
    return jax.shard_map(body, mesh=mesh, in_specs=in_specs, out_specs=out_specs, check_vma=False)
```

```python
import math

import jax
import jax.numpy as jnp
from jax import lax
from jax.experimental import pallas as pl
from jax.experimental.pallas import tpu as pltpu
from jax.sharding import PartitionSpec as P

TY = 4
FH = 3
STEPS = 2
ND = 36
PAD = 5
WIDE = ND + 2 * PAD
HALF = ND // 2
GROUP = 3
MESH = pl.DeviceIdType.MESH

weight_plus = 1.0 / 1.25**4
weight_minus = 1.0 / 0.75**4
weight_cross = 1.0 / (1.0 - 0.25**2) ** 4
source_step = 0.5

COS = [math.cos((j + 0.5) * 2.0 * math.pi / ND) for j in range(ND)]
SIN = [math.sin((j + 0.5) * 2.0 * math.pi / ND) for j in range(ND)]
EASTWARD = [j for j in range(ND) if COS[j] > 0]
WESTWARD = [j for j in range(ND) if COS[j] < 0]
NORTHWARD = [j for j in range(ND) if SIN[j] > 0]
SOUTHWARD = [j for j in range(ND) if SIN[j] < 0]


def kernel(
    n_k,
    back_in,
    tang_in,
    mask_hbm,
    coupling_hbm,
    freq_hbm,
    dir_hbm,
    back_out,
    tang_out,
    state_0,
    state_1,
    low_ext_0,
    low_ext_1,
    high_ext_0,
    high_ext_1,
    row_send,
    row_recv,
    col_send,
    col_recv,
    mask_in,
    coupling,
    freq_off,
    dir_off,
    speed,
    load_sem,
    small_sem,
    row_ssem,
    row_rsem,
    col_ssem,
    col_rsem,
    band_ssem,
    band_rsem,
):
    tiles = lax.axis_size("tile")
    bands = lax.axis_size("band")
    tile = lax.axis_index("tile")
    band = lax.axis_index("band")
    lat = lax.rem(tile + TY // 2, TY)
    north = lax.rem(tile + 1, tiles)
    south = lax.rem(tile + tiles - 1, tiles)
    east = lax.rem(tile + TY, tiles)
    west = lax.rem(tile + tiles - TY, tiles)
    has_north = lat < TY - 1
    has_south = lat > 0
    has_up = band < bands - 1
    has_down = band > 0
    groups = n_k // GROUP
    states = (state_0, state_1)
    low_exts = (low_ext_0, low_ext_1)
    high_exts = (high_ext_0, high_ext_1)
    inputs = (back_in, tang_in)
    outputs = (back_out, tang_out)

    def load_copy(f, g):
        return pltpu.make_async_copy(
            inputs[f].at[pl.ds(g * GROUP, GROUP), :, 0],
            state_0.at[f, pl.ds(g * GROUP, GROUP), pl.ds(PAD, ND)],
            load_sem.at[f, g],
        )

    small = [
        pltpu.make_async_copy(src, dst, small_sem.at[i])
        for i, (src, dst) in enumerate(
            (
                (mask_hbm, mask_in),
                (coupling_hbm, coupling),
                (freq_hbm, freq_off),
                (dir_hbm, dir_off),
            )
        )
    ]

    def row_copy(slot, side, g):
        ks = pl.ds(g * GROUP, GROUP)
        return pltpu.make_async_remote_copy(
            src_ref=row_send.at[slot, side, ks],
            dst_ref=row_recv.at[slot, side, ks],
            send_sem=row_ssem.at[slot, side, g],
            recv_sem=row_rsem.at[slot, side, g],
            device_id={"tile": north if side == 0 else south},
            device_id_type=MESH,
        )

    def col_copy(slot, side, g):
        return pltpu.make_async_remote_copy(
            src_ref=col_send.at[slot, side, g],
            dst_ref=col_recv.at[slot, side, g],
            send_sem=col_ssem.at[slot, side, g],
            recv_sem=col_rsem.at[slot, side, g],
            device_id={"tile": east if side == 0 else west},
            device_id_type=MESH,
        )

    def band_copy(step, side):
        if side == 0:
            src = states[step].at[:, pl.ds(n_k - FH, FH), pl.ds(PAD, ND)]
            dst = low_exts[step].at[:, pl.ds(0, FH), pl.ds(PAD, ND)]
            target = lax.rem(band + 1, bands)
        else:
            src = states[step].at[:, pl.ds(0, FH), pl.ds(PAD, ND)]
            dst = high_exts[step].at[:, pl.ds(FH - 1, FH), pl.ds(PAD, ND)]
            target = lax.rem(band + bands - 1, bands)
        return pltpu.make_async_remote_copy(
            src_ref=src,
            dst_ref=dst,
            send_sem=band_ssem.at[step, side],
            recv_sem=band_rsem.at[step, side],
            device_id={"band": target},
            device_id_type=MESH,
        )

    def send_halo(slot, g):
        @pl.when(has_north)
        def _():
            row_copy(slot, 0, g).start()

        @pl.when(has_south)
        def _():
            row_copy(slot, 1, g).start()

        col_copy(slot, 0, g).start()
        col_copy(slot, 1, g).start()

    def wait_halo(slot, g):
        @pl.when(has_south)
        def _():
            row_copy(slot, 0, g).wait_recv()

        @pl.when(has_north)
        def _():
            row_copy(slot, 1, g).wait_recv()

        col_copy(slot, 0, g).wait_recv()
        col_copy(slot, 1, g).wait_recv()

    for copy in small:
        copy.start()
    for g in (0, 2, 1):
        for f in range(2):
            load_copy(f, g).start()

    barrier = pltpu.get_barrier_semaphore()
    for cond, target in (
        (None, {"tile": east}),
        (None, {"tile": west}),
        (has_north, {"tile": north}),
        (has_south, {"tile": south}),
        (has_up, {"band": lax.rem(band + 1, bands)}),
        (has_down, {"band": lax.rem(band + bands - 1, bands)}),
    ):

        def greet(target=target):
            pl.semaphore_signal(barrier, inc=1, device_id=target, device_id_type=MESH)

        if cond is None:
            greet()
        else:
            pl.when(cond)(greet)

    base = jnp.float32(0.7)
    for b in range(1, 4):
        base = jnp.where(band == b, jnp.float32(0.7 * 1.1 ** (-n_k * b)), base)
    for k in range(n_k):
        speed[k] = base * jnp.float32(1.1 ** (-k))

    lane = lax.broadcasted_iota(jnp.int32, (8, 128), 1)
    sub = lax.broadcasted_iota(jnp.int32, (8, 128), 0)
    for copy in small:
        copy.wait()
    mask = mask_in[0].astype(jnp.float32)
    zeros = jnp.zeros((8, 128), jnp.float32)

    def zero_rows(side):
        def slots(i, _):
            row_recv[i // n_k, side, lax.rem(i, n_k)] = jnp.zeros((2, HALF, 128), jnp.float32)
            return 0

        lax.fori_loop(0, 2 * STEPS * n_k, slots, 0)

    pl.when(jnp.logical_not(has_south))(lambda: zero_rows(0))
    pl.when(jnp.logical_not(has_north))(lambda: zero_rows(1))

    def zero_ext(ext, first):
        def rows(r, _):
            ext[r // FH, first + lax.rem(r, FH)] = jnp.zeros((WIDE, 8, 128), jnp.float32)
            return 0

        lax.fori_loop(0, 2 * FH, rows, 0)

    for step in range(STEPS):
        pl.when(jnp.logical_not(has_down))(lambda: zero_ext(low_exts[step], 0))
        pl.when(jnp.logical_not(has_up))(lambda: zero_ext(high_exts[step], FH - 1))

    def pack_bin(f, kk, j, new, parts):
        if COS[j] > 0:
            c = kk * ND + f * HALF + EASTWARD.index(j)
            moved = pltpu.roll(new, (c + 1) % 128, 1)
            return [jnp.where(lane == c, moved, parts[0]), parts[1]]
        c = kk * ND + f * HALF + WESTWARD.index(j)
        moved = new if c == 0 else pltpu.roll(new, c, 1)
        return [parts[0], jnp.where(lane == c, moved, parts[1])]

    def finish_pack(state, slot, g, parts):
        rows = state.reshape(2, n_k, WIDE * 8, 128)
        for kk in range(GROUP):
            k = g * GROUP + kk
            for f in range(2):
                row_send[slot, 0, k, f] = rows[f, k, pl.ds(8 * PAD + 7, HALF, stride=8), :]
                row_send[slot, 1, k, f] = rows[f, k, pl.ds(8 * (PAD + HALF), HALF, stride=8), :]
        col_send[slot, 0, g] = parts[0]
        col_send[slot, 1, g] = parts[1]

    def write_state(step, f, k, j, new):
        state = states[step]
        state[f, k, PAD + j] = new
        if j >= ND - PAD:
            state[f, k, j - (ND - PAD)] = new
        if j < PAD:
            state[f, k, PAD + ND + j] = new

    def entry(i, _):
        g = lax.rem(2 * i, groups)

        for f in range(2):
            load_copy(f, g).wait()
        parts = [zeros, zeros]
        for kk in range(GROUP):
            k = g * GROUP + kk
            for f in range(2):
                for j in range(ND):
                    new = state_0[f, k, PAD + j] * mask
                    state_0[f, k, PAD + j] = new
                    parts = pack_bin(f, kk, j, new, parts)
        finish_pack(state_0, 0, g, parts)
        return 0

    lax.fori_loop(0, groups, entry, 0)

    peers = (
        2
        + has_north.astype(jnp.int32)
        + has_south.astype(jnp.int32)
        + has_up.astype(jnp.int32)
        + has_down.astype(jnp.int32)
    )
    pl.semaphore_wait(barrier, peers)

    for g in (0, 2, 1):
        send_halo(0, g)

    def substep(step, part):
        slot = 2 * step + part

        def group(i, _):
            g = lax.rem(2 * i + step, groups)
            wait_halo(slot, g)
            col_low = col_recv[slot, 0, g]
            col_high = col_recv[slot, 1, g]

            for kk in range(GROUP):
                k = g * GROUP + kk
                rate = speed[k]
                for j in range(ND):
                    rate_x = rate * jnp.float32(abs(COS[j]))
                    rate_y = rate * jnp.float32(abs(SIN[j]))
                    rate_0 = jnp.float32(1.0) - rate_x - rate_y
                    for f in range(2):
                        old = states[step][f, k, PAD + j]
                        if COS[j] > 0:
                            c = kk * ND + f * HALF + EASTWARD.index(j)
                            edge = col_low if c == 0 else pltpu.roll(col_low, 128 - c, 1)
                            side = jnp.where(lane == 0, edge, pltpu.roll(old, 1, 1))
                        else:
                            c = kk * ND + f * HALF + WESTWARD.index(j)
                            edge = pltpu.roll(col_high, 127 - c, 1)
                            side = jnp.where(lane == 127, edge, pltpu.roll(old, 127, 1))
                        r = j if SIN[j] > 0 else j - HALF
                        if SIN[j] > 0:
                            row = row_recv[slot, 0, k, f, pl.ds(r, 1), :]
                            above = jnp.where(sub == 0, row, pltpu.roll(old, 1, 0))
                        else:
                            row = row_recv[slot, 1, k, f, pl.ds(r, 1), :]
                            above = jnp.where(sub == 7, row, pltpu.roll(old, 7, 0))
                        new = mask * (rate_0 * old + rate_x * side + rate_y * above)
                        if part == 0:
                            states[step][f, k, PAD + j] = new
                        else:
                            write_state(step, f, k, j, new)
            if part == 0:

                @pl.when(g >= 0)
                def _():
                    parts = [zeros, zeros]
                    for kk in range(GROUP):
                        k = g * GROUP + kk
                        for f in range(2):
                            for j in range(ND):
                                parts = pack_bin(f, kk, j, states[step][f, k, PAD + j], parts)
                    finish_pack(states[step], slot + 1, g, parts)

                send_halo(slot + 1, g)
            else:

                @pl.when(jnp.logical_and(g == 0, has_down))
                def _():
                    band_copy(step, 1).start()

                @pl.when(jnp.logical_and(g == groups - 1, has_up))
                def _():
                    band_copy(step, 0).start()

            return 0

        lax.fori_loop(0, groups, group, 0)

    def wrap(ext, first):
        def one(i, _):
            f, k = i // FH, first + lax.rem(i, FH)
            ext[f, k, pl.ds(0, PAD)] = ext[f, k, pl.ds(ND, PAD)]
            ext[f, k, pl.ds(ND + PAD, PAD)] = ext[f, k, pl.ds(PAD, PAD)]
            return 0

        lax.fori_loop(0, 2 * FH, one, 0)

    def lend(ext, step, first, k0):
        def one(i, _):
            f, k = i // (FH - 1), lax.rem(i, FH - 1)
            ext[f, first + k] = states[step][f, k0 + k]
            return 0

        lax.fori_loop(0, 2 * (FH - 1), one, 0)

    def source(step, g, upper, lower):
        up = jnp.maximum(freq_off[0], 1)
        down = jnp.maximum(freq_off[1], 1)
        e = dir_off[0]
        h = dir_off[1]
        slot = 2 * step + 2

        parts = [zeros, zeros]
        for kk in range(GROUP):
            k = g * GROUP + kk
            strength = source_step * coupling[k]
            for j in range(ND):
                f0 = states[step][0, k, PAD + j]
                g0 = states[step][1, k, PAD + j]
                fp1, gp1 = upper(k + up, j + e)
                fm1, gm1 = lower(k - down, j - h)
                fp2, gp2 = upper(k + up, j - e)
                fm2, gm2 = lower(k - down, j + h)
                linear = weight_plus * (fp1 + fp2) + weight_minus * (fm1 + fm2)
                linear_t = weight_plus * (gp1 + gp2) + weight_minus * (gm1 + gm2)
                cross = weight_cross * (fp1 * fm1 + fp2 * fm2)
                cross_t = weight_cross * (gp1 * fm1 + fp1 * gm1 + gp2 * fm2 + fp2 * gm2)
                lead = f0 * linear
                rest = lead - cross
                rate = f0 * rest
                change = g0 * (lead + rest) + f0 * (f0 * linear_t - cross_t)
                for f, new in ((0, f0 - strength * rate), (1, g0 - strength * change)):
                    if step < STEPS - 1:
                        states[step + 1][f, k, PAD + j] = new
                        parts = pack_bin(f, kk, j, new, parts)
                    else:
                        outputs[f][k, j, 0] = new
        if step < STEPS - 1:
            finish_pack(states[step + 1], slot, g, parts)
            send_halo(slot, g)

    def model_step(step):
        low_ext, high_ext = low_exts[step], high_exts[step]
        substep(step, 0)
        substep(step, 1)

        def local(k, j):
            return states[step][0, k, PAD + j], states[step][1, k, PAD + j]

        def low(k, j):
            return low_ext[0, k + FH, PAD + j], low_ext[1, k + FH, PAD + j]

        def high(k, j):
            i = k - (n_k - FH + 1)
            return high_ext[0, i, PAD + j], high_ext[1, i, PAD + j]

        source(step, 1, local, local)
        lend(low_ext, step, FH, 0)
        lend(high_ext, step, 0, n_k - FH + 1)

        @pl.when(has_down)
        def _():
            band_copy(step, 0).wait_recv()
            wrap(low_ext, 0)

        source(step, 0, local, low)

        @pl.when(has_up)
        def _():
            band_copy(step, 1).wait_recv()
            wrap(high_ext, FH - 1)

        source(step, groups - 1, high, local)

    for step in range(STEPS):
        model_step(step)

    def drain(i, _):
        slot, g = i // groups, lax.rem(i, groups)

        @pl.when(has_north)
        def _():
            row_copy(slot, 0, g).wait_send()

        @pl.when(has_south)
        def _():
            row_copy(slot, 1, g).wait_send()

        col_copy(slot, 0, g).wait_send()
        col_copy(slot, 1, g).wait_send()
        return 0

    lax.fori_loop(0, 2 * STEPS * groups, drain, 0)
    for step in range(STEPS):

        @pl.when(has_up)
        def _():
            band_copy(step, 0).wait_send()

        @pl.when(has_down)
        def _():
            band_copy(step, 1).wait_send()


def body(background, tangent, sea_mask, coupling, freq_offsets, dir_offsets):
    n_k = background.shape[0]
    groups = n_k // GROUP
    slots = 2 * STEPS
    f32 = jnp.float32
    dma = pltpu.SemaphoreType.DMA
    out = jax.ShapeDtypeStruct(background.shape, f32)
    return pl.pallas_call(
        lambda *refs: kernel(n_k, *refs),
        out_shape=(out, out),
        in_specs=[pl.BlockSpec(memory_space=pltpu.HBM)] * 6,
        out_specs=(pl.BlockSpec(memory_space=pltpu.VMEM), pl.BlockSpec(memory_space=pltpu.VMEM)),
        scratch_shapes=[
            pltpu.VMEM((2, n_k, WIDE, 8, 128), f32),
            pltpu.VMEM((2, n_k, WIDE, 8, 128), f32),
            pltpu.VMEM((2, 2 * FH - 1, WIDE, 8, 128), f32),
            pltpu.VMEM((2, 2 * FH - 1, WIDE, 8, 128), f32),
            pltpu.VMEM((2, 2 * FH - 1, WIDE, 8, 128), f32),
            pltpu.VMEM((2, 2 * FH - 1, WIDE, 8, 128), f32),
            pltpu.VMEM((slots, 2, n_k, 2, HALF, 128), f32),
            pltpu.VMEM((slots, 2, n_k, 2, HALF, 128), f32),
            pltpu.VMEM((slots, 2, groups, 8, 128), f32),
            pltpu.VMEM((slots, 2, groups, 8, 128), f32),
            pltpu.VMEM((1, 8, 128), jnp.int32),
            pltpu.SMEM((n_k,), f32),
            pltpu.SMEM((2,), jnp.int32),
            pltpu.SMEM((2,), jnp.int32),
            pltpu.SMEM((n_k,), f32),
            dma((2, groups)),
            dma((4,)),
            dma((slots, 2, groups)),
            dma((slots, 2, groups)),
            dma((slots, 2, groups)),
            dma((slots, 2, groups)),
            dma((STEPS, 2)),
            dma((STEPS, 2)),
        ],
        compiler_params=pltpu.CompilerParams(
            collective_id=0, has_side_effects=True, vmem_limit_bytes=48 * 1024 * 1024
        ),
        name="wave_steps",
    )(*[pltpu.with_memory_space_constraint(x, pltpu.HBM) for x in (background, tangent, sea_mask, coupling, freq_offsets, dir_offsets)])


def solution(mesh):
    in_specs = (
        P("band", None, "tile", None, None),
        P("band", None, "tile", None, None),
        P("tile", None, None),
        P("band"),
        P(),
        P(),
    )
    out_specs = (P("band", None, "tile", None, None), P("band", None, "tile", None, None))
    return jax.shard_map(body, mesh=mesh, in_specs=in_specs, out_specs=out_specs, check_vma=False)
```

```python
import math

import jax
import jax.numpy as jnp
from jax import lax
from jax.experimental import pallas as pl
from jax.experimental.pallas import tpu as pltpu
from jax.sharding import PartitionSpec as P

TY = 4
FH = 3
STEPS = 2
ND = 36
PAD = 5
WIDE = ND + 2 * PAD
HALF = ND // 2
GROUP = 3
MESH = pl.DeviceIdType.MESH

weight_plus = 1.0 / 1.25**4
weight_minus = 1.0 / 0.75**4
weight_cross = 1.0 / (1.0 - 0.25**2) ** 4
source_step = 0.5

COS = [math.cos((j + 0.5) * 2.0 * math.pi / ND) for j in range(ND)]
SIN = [math.sin((j + 0.5) * 2.0 * math.pi / ND) for j in range(ND)]
EASTWARD = [j for j in range(ND) if COS[j] > 0]
WESTWARD = [j for j in range(ND) if COS[j] < 0]
NORTHWARD = [j for j in range(ND) if SIN[j] > 0]
SOUTHWARD = [j for j in range(ND) if SIN[j] < 0]


def kernel(
    n_k,
    back_in,
    tang_in,
    mask_hbm,
    coupling_hbm,
    freq_hbm,
    dir_hbm,
    back_out,
    tang_out,
    state_0,
    state_1,
    low_ext_0,
    low_ext_1,
    high_ext_0,
    high_ext_1,
    row_send,
    row_recv,
    col_send,
    col_recv,
    mask_in,
    coupling,
    freq_off,
    dir_off,
    speed,
    load_sem,
    small_sem,
    row_ssem,
    row_rsem,
    col_ssem,
    col_rsem,
    band_ssem,
    band_rsem,
):
    tiles = lax.axis_size("tile")
    bands = lax.axis_size("band")
    tile = lax.axis_index("tile")
    band = lax.axis_index("band")
    lat = lax.rem(tile + TY // 2, TY)
    north = lax.rem(tile + 1, tiles)
    south = lax.rem(tile + tiles - 1, tiles)
    east = lax.rem(tile + TY, tiles)
    west = lax.rem(tile + tiles - TY, tiles)
    has_north = lat < TY - 1
    has_south = lat > 0
    has_up = band < bands - 1
    has_down = band > 0
    groups = n_k // GROUP
    first = jnp.where(band < bands // 2, groups - 1, 0)
    second = groups - 1 - first

    def urgent(i):
        return jnp.where(i == 0, first, jnp.where(i == 1, second, 1))

    def arrival(i):
        return jnp.where(i == 0, 1, jnp.where(i == 1, second, first))

    states = (state_0, state_1)
    low_exts = (low_ext_0, low_ext_1)
    high_exts = (high_ext_0, high_ext_1)
    inputs = (back_in, tang_in)
    outputs = (back_out, tang_out)

    def load_copy(f, g):
        return pltpu.make_async_copy(
            inputs[f].at[pl.ds(g * GROUP, GROUP), :, 0],
            state_0.at[f, pl.ds(g * GROUP, GROUP), pl.ds(PAD, ND)],
            load_sem.at[f, g],
        )

    small = [
        pltpu.make_async_copy(src, dst, small_sem.at[i])
        for i, (src, dst) in enumerate(
            (
                (mask_hbm, mask_in),
                (coupling_hbm, coupling),
                (freq_hbm, freq_off),
                (dir_hbm, dir_off),
            )
        )
    ]

    def row_copy(slot, side, g):
        ks = pl.ds(g * GROUP, GROUP)
        return pltpu.make_async_remote_copy(
            src_ref=row_send.at[slot, side, ks],
            dst_ref=row_recv.at[slot, side, ks],
            send_sem=row_ssem.at[slot, side, g],
            recv_sem=row_rsem.at[slot, side, g],
            device_id={"tile": north if side == 0 else south},
            device_id_type=MESH,
        )

    def col_copy(slot, side, g):
        return pltpu.make_async_remote_copy(
            src_ref=col_send.at[slot, side, g],
            dst_ref=col_recv.at[slot, side, g],
            send_sem=col_ssem.at[slot, side, g],
            recv_sem=col_rsem.at[slot, side, g],
            device_id={"tile": east if side == 0 else west},
            device_id_type=MESH,
        )

    def band_copy(step, side):
        if side == 0:
            src = states[step].at[:, pl.ds(n_k - FH, FH), pl.ds(PAD, ND)]
            dst = low_exts[step].at[:, pl.ds(0, FH), pl.ds(PAD, ND)]
            target = lax.rem(band + 1, bands)
        else:
            src = states[step].at[:, pl.ds(0, FH), pl.ds(PAD, ND)]
            dst = high_exts[step].at[:, pl.ds(FH - 1, FH), pl.ds(PAD, ND)]
            target = lax.rem(band + bands - 1, bands)
        return pltpu.make_async_remote_copy(
            src_ref=src,
            dst_ref=dst,
            send_sem=band_ssem.at[step, side],
            recv_sem=band_rsem.at[step, side],
            device_id={"band": target},
            device_id_type=MESH,
        )

    def send_halo(slot, g):
        @pl.when(has_north)
        def _():
            row_copy(slot, 0, g).start()

        @pl.when(has_south)
        def _():
            row_copy(slot, 1, g).start()

        col_copy(slot, 0, g).start()
        col_copy(slot, 1, g).start()

    def wait_halo(slot, g):
        @pl.when(has_south)
        def _():
            row_copy(slot, 0, g).wait_recv()

        @pl.when(has_north)
        def _():
            row_copy(slot, 1, g).wait_recv()

        col_copy(slot, 0, g).wait_recv()
        col_copy(slot, 1, g).wait_recv()

    for copy in small:
        copy.start()
    for g in (0, 2, 1):
        for f in range(2):
            load_copy(f, g).start()

    barrier = pltpu.get_barrier_semaphore()
    for cond, target in (
        (None, {"tile": east}),
        (None, {"tile": west}),
        (has_north, {"tile": north}),
        (has_south, {"tile": south}),
        (has_up, {"band": lax.rem(band + 1, bands)}),
        (has_down, {"band": lax.rem(band + bands - 1, bands)}),
    ):

        def greet(target=target):
            pl.semaphore_signal(barrier, inc=1, device_id=target, device_id_type=MESH)

        if cond is None:
            greet()
        else:
            pl.when(cond)(greet)

    base = jnp.float32(0.7)
    for b in range(1, 4):
        base = jnp.where(band == b, jnp.float32(0.7 * 1.1 ** (-n_k * b)), base)
    for k in range(n_k):
        speed[k] = base * jnp.float32(1.1 ** (-k))

    lane = lax.broadcasted_iota(jnp.int32, (8, 128), 1)
    sub = lax.broadcasted_iota(jnp.int32, (8, 128), 0)
    for copy in small:
        copy.wait()
    mask = mask_in[0].astype(jnp.float32)
    zeros = jnp.zeros((8, 128), jnp.float32)

    def zero_rows(side):
        def slots(i, _):
            row_recv[i // n_k, side, lax.rem(i, n_k)] = jnp.zeros((2, HALF, 128), jnp.float32)
            return 0

        lax.fori_loop(0, 2 * STEPS * n_k, slots, 0)

    pl.when(jnp.logical_not(has_south))(lambda: zero_rows(0))
    pl.when(jnp.logical_not(has_north))(lambda: zero_rows(1))

    def zero_ext(ext, first):
        def rows(r, _):
            ext[r // FH, first + lax.rem(r, FH)] = jnp.zeros((WIDE, 8, 128), jnp.float32)
            return 0

        lax.fori_loop(0, 2 * FH, rows, 0)

    for step in range(STEPS):
        pl.when(jnp.logical_not(has_down))(lambda: zero_ext(low_exts[step], 0))
        pl.when(jnp.logical_not(has_up))(lambda: zero_ext(high_exts[step], FH - 1))

    def pack_bin(f, kk, j, new, parts):
        if COS[j] > 0:
            c = kk * ND + f * HALF + EASTWARD.index(j)
            moved = pltpu.roll(new, (c + 1) % 128, 1)
            return [jnp.where(lane == c, moved, parts[0]), parts[1]]
        c = kk * ND + f * HALF + WESTWARD.index(j)
        moved = new if c == 0 else pltpu.roll(new, c, 1)
        return [parts[0], jnp.where(lane == c, moved, parts[1])]

    def finish_pack(state, slot, g, parts):
        rows = state.reshape(2, n_k, WIDE * 8, 128)
        for kk in range(GROUP):
            k = g * GROUP + kk
            for f in range(2):
                row_send[slot, 0, k, f] = rows[f, k, pl.ds(8 * PAD + 7, HALF, stride=8), :]
                row_send[slot, 1, k, f] = rows[f, k, pl.ds(8 * (PAD + HALF), HALF, stride=8), :]
        col_send[slot, 0, g] = parts[0]
        col_send[slot, 1, g] = parts[1]

    def write_state(step, f, k, j, new):
        state = states[step]
        state[f, k, PAD + j] = new
        if j >= ND - PAD:
            state[f, k, j - (ND - PAD)] = new
        if j < PAD:
            state[f, k, PAD + ND + j] = new

    def entry(i, _):
        g = urgent(i)

        for f in range(2):
            load_copy(f, g).wait()
        parts = [zeros, zeros]
        for kk in range(GROUP):
            k = g * GROUP + kk
            for f in range(2):
                for j in range(ND):
                    new = state_0[f, k, PAD + j] * mask
                    state_0[f, k, PAD + j] = new
                    parts = pack_bin(f, kk, j, new, parts)
        finish_pack(state_0, 0, g, parts)
        return 0

    lax.fori_loop(0, groups, entry, 0)

    peers = (
        2
        + has_north.astype(jnp.int32)
        + has_south.astype(jnp.int32)
        + has_up.astype(jnp.int32)
        + has_down.astype(jnp.int32)
    )
    pl.semaphore_wait(barrier, peers)

    for i in range(groups):
        send_halo(0, urgent(i))

    def substep(step, part):
        slot = 2 * step + part

        def group(i, _):
            g = arrival(i) if slot == 2 else urgent(i)
            wait_halo(slot, g)
            col_low = col_recv[slot, 0, g]
            col_high = col_recv[slot, 1, g]

            for kk in range(GROUP):
                k = g * GROUP + kk
                rate = speed[k]
                for j in range(ND):
                    rate_x = rate * jnp.float32(abs(COS[j]))
                    rate_y = rate * jnp.float32(abs(SIN[j]))
                    rate_0 = jnp.float32(1.0) - rate_x - rate_y
                    for f in range(2):
                        old = states[step][f, k, PAD + j]
                        if COS[j] > 0:
                            c = kk * ND + f * HALF + EASTWARD.index(j)
                            edge = col_low if c == 0 else pltpu.roll(col_low, 128 - c, 1)
                            side = jnp.where(lane == 0, edge, pltpu.roll(old, 1, 1))
                        else:
                            c = kk * ND + f * HALF + WESTWARD.index(j)
                            edge = pltpu.roll(col_high, 127 - c, 1)
                            side = jnp.where(lane == 127, edge, pltpu.roll(old, 127, 1))
                        r = j if SIN[j] > 0 else j - HALF
                        if SIN[j] > 0:
                            row = row_recv[slot, 0, k, f, pl.ds(r, 1), :]
                            above = jnp.where(sub == 0, row, pltpu.roll(old, 1, 0))
                        else:
                            row = row_recv[slot, 1, k, f, pl.ds(r, 1), :]
                            above = jnp.where(sub == 7, row, pltpu.roll(old, 7, 0))
                        new = mask * (rate_0 * old + rate_x * side + rate_y * above)
                        if part == 0:
                            states[step][f, k, PAD + j] = new
                        else:
                            write_state(step, f, k, j, new)
            if part == 0:

                @pl.when(g >= 0)
                def _():
                    parts = [zeros, zeros]
                    for kk in range(GROUP):
                        k = g * GROUP + kk
                        for f in range(2):
                            for j in range(ND):
                                parts = pack_bin(f, kk, j, states[step][f, k, PAD + j], parts)
                    finish_pack(states[step], slot + 1, g, parts)

                send_halo(slot + 1, g)
            else:

                @pl.when(jnp.logical_and(g == 0, has_down))
                def _():
                    band_copy(step, 1).start()

                @pl.when(jnp.logical_and(g == groups - 1, has_up))
                def _():
                    band_copy(step, 0).start()

            return 0

        lax.fori_loop(0, groups, group, 0)

    def wrap(ext, first):
        def one(i, _):
            f, k = i // FH, first + lax.rem(i, FH)
            ext[f, k, pl.ds(0, PAD)] = ext[f, k, pl.ds(ND, PAD)]
            ext[f, k, pl.ds(ND + PAD, PAD)] = ext[f, k, pl.ds(PAD, PAD)]
            return 0

        lax.fori_loop(0, 2 * FH, one, 0)

    def lend(ext, step, first, k0):
        def one(i, _):
            f, k = i // (FH - 1), lax.rem(i, FH - 1)
            ext[f, first + k] = states[step][f, k0 + k]
            return 0

        lax.fori_loop(0, 2 * (FH - 1), one, 0)

    def source(step, g, upper, lower):
        up = jnp.maximum(freq_off[0], 1)
        down = jnp.maximum(freq_off[1], 1)
        e = dir_off[0]
        h = dir_off[1]
        slot = 2 * step + 2

        parts = [zeros, zeros]
        for kk in range(GROUP):
            k = g * GROUP + kk
            strength = source_step * coupling[k]
            for j in range(ND):
                f0 = states[step][0, k, PAD + j]
                g0 = states[step][1, k, PAD + j]
                fp1, gp1 = upper(k + up, j + e)
                fm1, gm1 = lower(k - down, j - h)
                fp2, gp2 = upper(k + up, j - e)
                fm2, gm2 = lower(k - down, j + h)
                linear = weight_plus * (fp1 + fp2) + weight_minus * (fm1 + fm2)
                linear_t = weight_plus * (gp1 + gp2) + weight_minus * (gm1 + gm2)
                cross = weight_cross * (fp1 * fm1 + fp2 * fm2)
                cross_t = weight_cross * (gp1 * fm1 + fp1 * gm1 + gp2 * fm2 + fp2 * gm2)
                lead = f0 * linear
                rest = lead - cross
                rate = f0 * rest
                change = g0 * (lead + rest) + f0 * (f0 * linear_t - cross_t)
                for f, new in ((0, f0 - strength * rate), (1, g0 - strength * change)):
                    if step < STEPS - 1:
                        states[step + 1][f, k, PAD + j] = new
                        parts = pack_bin(f, kk, j, new, parts)
                    else:
                        outputs[f][k, j, 0] = new
        if step < STEPS - 1:
            finish_pack(states[step + 1], slot, g, parts)
            send_halo(slot, g)

    def model_step(step):
        low_ext, high_ext = low_exts[step], high_exts[step]
        substep(step, 0)
        substep(step, 1)

        def local(k, j):
            return states[step][0, k, PAD + j], states[step][1, k, PAD + j]

        def low(k, j):
            return low_ext[0, k + FH, PAD + j], low_ext[1, k + FH, PAD + j]

        def high(k, j):
            i = k - (n_k - FH + 1)
            return high_ext[0, i, PAD + j], high_ext[1, i, PAD + j]

        source(step, 1, local, local)
        lend(low_ext, step, FH, 0)
        lend(high_ext, step, 0, n_k - FH + 1)

        def edge(i, _):
            is_low = jnp.where(i == 0, second, first) == 0

            @pl.when(jnp.logical_and(is_low, has_down))
            def _():
                band_copy(step, 0).wait_recv()
                wrap(low_ext, 0)

            @pl.when(is_low)
            def _():
                source(step, 0, local, low)

            is_high = jnp.logical_not(is_low)

            @pl.when(jnp.logical_and(is_high, has_up))
            def _():
                band_copy(step, 1).wait_recv()
                wrap(high_ext, FH - 1)

            @pl.when(is_high)
            def _():
                source(step, groups - 1, high, local)

            return 0

        lax.fori_loop(0, 2, edge, 0)

    for step in range(STEPS):
        model_step(step)

    def drain(i, _):
        slot, g = i // groups, lax.rem(i, groups)

        @pl.when(has_north)
        def _():
            row_copy(slot, 0, g).wait_send()

        @pl.when(has_south)
        def _():
            row_copy(slot, 1, g).wait_send()

        col_copy(slot, 0, g).wait_send()
        col_copy(slot, 1, g).wait_send()
        return 0

    lax.fori_loop(0, 2 * STEPS * groups, drain, 0)
    for step in range(STEPS):

        @pl.when(has_up)
        def _():
            band_copy(step, 0).wait_send()

        @pl.when(has_down)
        def _():
            band_copy(step, 1).wait_send()


def body(background, tangent, sea_mask, coupling, freq_offsets, dir_offsets):
    n_k = background.shape[0]
    groups = n_k // GROUP
    slots = 2 * STEPS
    f32 = jnp.float32
    dma = pltpu.SemaphoreType.DMA
    out = jax.ShapeDtypeStruct(background.shape, f32)
    return pl.pallas_call(
        lambda *refs: kernel(n_k, *refs),
        out_shape=(out, out),
        in_specs=[pl.BlockSpec(memory_space=pltpu.HBM)] * 6,
        out_specs=(pl.BlockSpec(memory_space=pltpu.VMEM), pl.BlockSpec(memory_space=pltpu.VMEM)),
        scratch_shapes=[
            pltpu.VMEM((2, n_k, WIDE, 8, 128), f32),
            pltpu.VMEM((2, n_k, WIDE, 8, 128), f32),
            pltpu.VMEM((2, 2 * FH - 1, WIDE, 8, 128), f32),
            pltpu.VMEM((2, 2 * FH - 1, WIDE, 8, 128), f32),
            pltpu.VMEM((2, 2 * FH - 1, WIDE, 8, 128), f32),
            pltpu.VMEM((2, 2 * FH - 1, WIDE, 8, 128), f32),
            pltpu.VMEM((slots, 2, n_k, 2, HALF, 128), f32),
            pltpu.VMEM((slots, 2, n_k, 2, HALF, 128), f32),
            pltpu.VMEM((slots, 2, groups, 8, 128), f32),
            pltpu.VMEM((slots, 2, groups, 8, 128), f32),
            pltpu.VMEM((1, 8, 128), jnp.int32),
            pltpu.SMEM((n_k,), f32),
            pltpu.SMEM((2,), jnp.int32),
            pltpu.SMEM((2,), jnp.int32),
            pltpu.SMEM((n_k,), f32),
            dma((2, groups)),
            dma((4,)),
            dma((slots, 2, groups)),
            dma((slots, 2, groups)),
            dma((slots, 2, groups)),
            dma((slots, 2, groups)),
            dma((STEPS, 2)),
            dma((STEPS, 2)),
        ],
        compiler_params=pltpu.CompilerParams(
            collective_id=0, has_side_effects=True, vmem_limit_bytes=48 * 1024 * 1024
        ),
        name="wave_steps",
    )(*[pltpu.with_memory_space_constraint(x, pltpu.HBM) for x in (background, tangent, sea_mask, coupling, freq_offsets, dir_offsets)])


def solution(mesh):
    in_specs = (
        P("band", None, "tile", None, None),
        P("band", None, "tile", None, None),
        P("tile", None, None),
        P("band"),
        P(),
        P(),
    )
    out_specs = (P("band", None, "tile", None, None), P("band", None, "tile", None, None))
    return jax.shard_map(body, mesh=mesh, in_specs=in_specs, out_specs=out_specs, check_vma=False)
```

```python
import math

import jax
import jax.numpy as jnp
from jax import lax
from jax.experimental import pallas as pl
from jax.experimental.pallas import tpu as pltpu
from jax.sharding import PartitionSpec as P

TY = 4
FH = 3
STEPS = 2
ND = 36
PAD = 5
WIDE = ND + 2 * PAD
HALF = ND // 2
GROUP = 3
MESH = pl.DeviceIdType.MESH

weight_plus = 1.0 / 1.25**4
weight_minus = 1.0 / 0.75**4
weight_cross = 1.0 / (1.0 - 0.25**2) ** 4
source_step = 0.5

COS = [math.cos((j + 0.5) * 2.0 * math.pi / ND) for j in range(ND)]
SIN = [math.sin((j + 0.5) * 2.0 * math.pi / ND) for j in range(ND)]
EASTWARD = [j for j in range(ND) if COS[j] > 0]
WESTWARD = [j for j in range(ND) if COS[j] < 0]
NORTHWARD = [j for j in range(ND) if SIN[j] > 0]
SOUTHWARD = [j for j in range(ND) if SIN[j] < 0]


def kernel(
    n_k,
    back_in,
    tang_in,
    mask_hbm,
    coupling_hbm,
    freq_hbm,
    dir_hbm,
    back_out,
    tang_out,
    state_0,
    state_1,
    low_ext_0,
    low_ext_1,
    high_ext_0,
    high_ext_1,
    row_send,
    row_recv,
    col_send,
    col_recv,
    mask_in,
    coupling,
    freq_off,
    dir_off,
    speed,
    load_sem,
    small_sem,
    row_ssem,
    row_rsem,
    col_ssem,
    col_rsem,
    band_ssem,
    band_rsem,
):
    tiles = lax.axis_size("tile")
    bands = lax.axis_size("band")
    tile = lax.axis_index("tile")
    band = lax.axis_index("band")
    lat = lax.rem(tile + TY // 2, TY)
    north = lax.rem(tile + 1, tiles)
    south = lax.rem(tile + tiles - 1, tiles)
    east = lax.rem(tile + TY, tiles)
    west = lax.rem(tile + tiles - TY, tiles)
    has_north = lat < TY - 1
    has_south = lat > 0
    has_up = band < bands - 1
    has_down = band > 0
    groups = n_k // GROUP
    first = jnp.where(band < bands // 2, groups - 1, 0)
    second = groups - 1 - first

    def urgent(i):
        return jnp.where(i == 0, first, jnp.where(i == 1, second, 1))

    def arrival(i):
        return jnp.where(i == 0, second, jnp.where(i == 1, first, 1))

    states = (state_0, state_1)
    low_exts = (low_ext_0, low_ext_1)
    high_exts = (high_ext_0, high_ext_1)
    inputs = (back_in, tang_in)
    outputs = (back_out, tang_out)

    def load_copy(f, g):
        return pltpu.make_async_copy(
            inputs[f].at[pl.ds(g * GROUP, GROUP), :, 0],
            state_0.at[f, pl.ds(g * GROUP, GROUP), pl.ds(PAD, ND)],
            load_sem.at[f, g],
        )

    small = [
        pltpu.make_async_copy(src, dst, small_sem.at[i])
        for i, (src, dst) in enumerate(
            (
                (mask_hbm, mask_in),
                (coupling_hbm, coupling),
                (freq_hbm, freq_off),
                (dir_hbm, dir_off),
            )
        )
    ]

    def row_copy(slot, side, g):
        ks = pl.ds(g * GROUP, GROUP)
        return pltpu.make_async_remote_copy(
            src_ref=row_send.at[slot, side, ks],
            dst_ref=row_recv.at[slot, side, ks],
            send_sem=row_ssem.at[slot, side, g],
            recv_sem=row_rsem.at[slot, side, g],
            device_id={"tile": north if side == 0 else south},
            device_id_type=MESH,
        )

    def col_copy(slot, side, g):
        return pltpu.make_async_remote_copy(
            src_ref=col_send.at[slot, side, g],
            dst_ref=col_recv.at[slot, side, g],
            send_sem=col_ssem.at[slot, side, g],
            recv_sem=col_rsem.at[slot, side, g],
            device_id={"tile": east if side == 0 else west},
            device_id_type=MESH,
        )

    def band_copy(step, side):
        if side == 0:
            src = states[step].at[:, pl.ds(n_k - FH, FH), pl.ds(PAD, ND)]
            dst = low_exts[step].at[:, pl.ds(0, FH), pl.ds(PAD, ND)]
            target = lax.rem(band + 1, bands)
        else:
            src = states[step].at[:, pl.ds(0, FH), pl.ds(PAD, ND)]
            dst = high_exts[step].at[:, pl.ds(FH - 1, FH), pl.ds(PAD, ND)]
            target = lax.rem(band + bands - 1, bands)
        return pltpu.make_async_remote_copy(
            src_ref=src,
            dst_ref=dst,
            send_sem=band_ssem.at[step, side],
            recv_sem=band_rsem.at[step, side],
            device_id={"band": target},
            device_id_type=MESH,
        )

    def send_halo(slot, g):
        @pl.when(has_north)
        def _():
            row_copy(slot, 0, g).start()

        @pl.when(has_south)
        def _():
            row_copy(slot, 1, g).start()

        col_copy(slot, 0, g).start()
        col_copy(slot, 1, g).start()

    def wait_halo(slot, g):
        @pl.when(has_south)
        def _():
            row_copy(slot, 0, g).wait_recv()

        @pl.when(has_north)
        def _():
            row_copy(slot, 1, g).wait_recv()

        col_copy(slot, 0, g).wait_recv()
        col_copy(slot, 1, g).wait_recv()

    for copy in small:
        copy.start()
    for g in (0, 2, 1):
        for f in range(2):
            load_copy(f, g).start()

    barrier = pltpu.get_barrier_semaphore()
    for cond, target in (
        (None, {"tile": east}),
        (None, {"tile": west}),
        (has_north, {"tile": north}),
        (has_south, {"tile": south}),
        (has_up, {"band": lax.rem(band + 1, bands)}),
        (has_down, {"band": lax.rem(band + bands - 1, bands)}),
    ):

        def greet(target=target):
            pl.semaphore_signal(barrier, inc=1, device_id=target, device_id_type=MESH)

        if cond is None:
            greet()
        else:
            pl.when(cond)(greet)

    base = jnp.float32(0.7)
    for b in range(1, 4):
        base = jnp.where(band == b, jnp.float32(0.7 * 1.1 ** (-n_k * b)), base)
    for k in range(n_k):
        speed[k] = base * jnp.float32(1.1 ** (-k))

    lane = lax.broadcasted_iota(jnp.int32, (8, 128), 1)
    sub = lax.broadcasted_iota(jnp.int32, (8, 128), 0)
    for copy in small:
        copy.wait()
    mask = mask_in[0].astype(jnp.float32)
    zeros = jnp.zeros((8, 128), jnp.float32)

    def zero_rows(side):
        def slots(i, _):
            row_recv[i // n_k, side, lax.rem(i, n_k)] = jnp.zeros((2, HALF, 128), jnp.float32)
            return 0

        lax.fori_loop(0, 2 * STEPS * n_k, slots, 0)

    pl.when(jnp.logical_not(has_south))(lambda: zero_rows(0))
    pl.when(jnp.logical_not(has_north))(lambda: zero_rows(1))

    def zero_ext(ext, first):
        def rows(r, _):
            ext[r // FH, first + lax.rem(r, FH)] = jnp.zeros((WIDE, 8, 128), jnp.float32)
            return 0

        lax.fori_loop(0, 2 * FH, rows, 0)

    for step in range(STEPS):
        pl.when(jnp.logical_not(has_down))(lambda: zero_ext(low_exts[step], 0))
        pl.when(jnp.logical_not(has_up))(lambda: zero_ext(high_exts[step], FH - 1))

    def pack_bin(f, kk, j, new, parts):
        if COS[j] > 0:
            c = kk * ND + f * HALF + EASTWARD.index(j)
            moved = pltpu.roll(new, (c + 1) % 128, 1)
            return [jnp.where(lane == c, moved, parts[0]), parts[1]]
        c = kk * ND + f * HALF + WESTWARD.index(j)
        moved = new if c == 0 else pltpu.roll(new, c, 1)
        return [parts[0], jnp.where(lane == c, moved, parts[1])]

    def finish_pack(state, slot, g, parts):
        rows = state.reshape(2, n_k, WIDE * 8, 128)
        for kk in range(GROUP):
            k = g * GROUP + kk
            for f in range(2):
                row_send[slot, 0, k, f] = rows[f, k, pl.ds(8 * PAD + 7, HALF, stride=8), :]
                row_send[slot, 1, k, f] = rows[f, k, pl.ds(8 * (PAD + HALF), HALF, stride=8), :]
        col_send[slot, 0, g] = parts[0]
        col_send[slot, 1, g] = parts[1]

    def write_state(step, f, k, j, new):
        state = states[step]
        state[f, k, PAD + j] = new
        if j >= ND - PAD:
            state[f, k, j - (ND - PAD)] = new
        if j < PAD:
            state[f, k, PAD + ND + j] = new

    def entry(i, _):
        g = urgent(i)

        for f in range(2):
            load_copy(f, g).wait()
        parts = [zeros, zeros]
        for kk in range(GROUP):
            k = g * GROUP + kk
            for f in range(2):
                for j in range(ND):
                    new = state_0[f, k, PAD + j] * mask
                    state_0[f, k, PAD + j] = new
                    parts = pack_bin(f, kk, j, new, parts)
        finish_pack(state_0, 0, g, parts)
        return 0

    lax.fori_loop(0, groups, entry, 0)

    peers = (
        2
        + has_north.astype(jnp.int32)
        + has_south.astype(jnp.int32)
        + has_up.astype(jnp.int32)
        + has_down.astype(jnp.int32)
    )
    pl.semaphore_wait(barrier, peers)

    for i in range(groups):
        send_halo(0, urgent(i))

    def substep(step, part):
        slot = 2 * step + part

        def group(i, _):
            g = arrival(i) if slot == 2 else urgent(i)
            wait_halo(slot, g)
            col_low = col_recv[slot, 0, g]
            col_high = col_recv[slot, 1, g]

            for kk in range(GROUP):
                k = g * GROUP + kk
                rate = speed[k]
                for j in range(ND):
                    rate_x = rate * jnp.float32(abs(COS[j]))
                    rate_y = rate * jnp.float32(abs(SIN[j]))
                    rate_0 = jnp.float32(1.0) - rate_x - rate_y
                    for f in range(2):
                        old = states[step][f, k, PAD + j]
                        if COS[j] > 0:
                            c = kk * ND + f * HALF + EASTWARD.index(j)
                            edge = col_low if c == 0 else pltpu.roll(col_low, 128 - c, 1)
                            side = jnp.where(lane == 0, edge, pltpu.roll(old, 1, 1))
                        else:
                            c = kk * ND + f * HALF + WESTWARD.index(j)
                            edge = pltpu.roll(col_high, 127 - c, 1)
                            side = jnp.where(lane == 127, edge, pltpu.roll(old, 127, 1))
                        r = j if SIN[j] > 0 else j - HALF
                        if SIN[j] > 0:
                            row = row_recv[slot, 0, k, f, pl.ds(r, 1), :]
                            above = jnp.where(sub == 0, row, pltpu.roll(old, 1, 0))
                        else:
                            row = row_recv[slot, 1, k, f, pl.ds(r, 1), :]
                            above = jnp.where(sub == 7, row, pltpu.roll(old, 7, 0))
                        new = mask * (rate_0 * old + rate_x * side + rate_y * above)
                        if part == 0:
                            states[step][f, k, PAD + j] = new
                        else:
                            write_state(step, f, k, j, new)
            if part == 0:

                @pl.when(g >= 0)
                def _():
                    parts = [zeros, zeros]
                    for kk in range(GROUP):
                        k = g * GROUP + kk
                        for f in range(2):
                            for j in range(ND):
                                parts = pack_bin(f, kk, j, states[step][f, k, PAD + j], parts)
                    finish_pack(states[step], slot + 1, g, parts)

                send_halo(slot + 1, g)
            else:

                @pl.when(jnp.logical_and(g == 0, has_down))
                def _():
                    band_copy(step, 1).start()

                @pl.when(jnp.logical_and(g == groups - 1, has_up))
                def _():
                    band_copy(step, 0).start()

            return 0

        lax.fori_loop(0, groups, group, 0)

    def wrap(ext, first):
        def one(i, _):
            f, k = i // FH, first + lax.rem(i, FH)
            ext[f, k, pl.ds(0, PAD)] = ext[f, k, pl.ds(ND, PAD)]
            ext[f, k, pl.ds(ND + PAD, PAD)] = ext[f, k, pl.ds(PAD, PAD)]
            return 0

        lax.fori_loop(0, 2 * FH, one, 0)

    def lend(ext, step, first, k0):
        def one(i, _):
            f, k = i // (FH - 1), lax.rem(i, FH - 1)
            ext[f, first + k] = states[step][f, k0 + k]
            return 0

        lax.fori_loop(0, 2 * (FH - 1), one, 0)

    def source(step, g, upper, lower):
        up = jnp.maximum(freq_off[0], 1)
        down = jnp.maximum(freq_off[1], 1)
        e = dir_off[0]
        h = dir_off[1]
        slot = 2 * step + 2

        parts = [zeros, zeros]
        for kk in range(GROUP):
            k = g * GROUP + kk
            strength = source_step * coupling[k]
            for j in range(ND):
                f0 = states[step][0, k, PAD + j]
                g0 = states[step][1, k, PAD + j]
                fp1, gp1 = upper(k + up, j + e)
                fm1, gm1 = lower(k - down, j - h)
                fp2, gp2 = upper(k + up, j - e)
                fm2, gm2 = lower(k - down, j + h)
                linear = weight_plus * (fp1 + fp2) + weight_minus * (fm1 + fm2)
                linear_t = weight_plus * (gp1 + gp2) + weight_minus * (gm1 + gm2)
                cross = weight_cross * (fp1 * fm1 + fp2 * fm2)
                cross_t = weight_cross * (gp1 * fm1 + fp1 * gm1 + gp2 * fm2 + fp2 * gm2)
                lead = f0 * linear
                rest = lead - cross
                rate = f0 * rest
                change = g0 * (lead + rest) + f0 * (f0 * linear_t - cross_t)
                for f, new in ((0, f0 - strength * rate), (1, g0 - strength * change)):
                    if step < STEPS - 1:
                        states[step + 1][f, k, PAD + j] = new
                        parts = pack_bin(f, kk, j, new, parts)
                    else:
                        outputs[f][k, j, 0] = new
        if step < STEPS - 1:
            finish_pack(states[step + 1], slot, g, parts)
            if g != 1:
                send_halo(slot, g)

    def model_step(step):
        low_ext, high_ext = low_exts[step], high_exts[step]
        substep(step, 0)
        substep(step, 1)

        def local(k, j):
            return states[step][0, k, PAD + j], states[step][1, k, PAD + j]

        def low(k, j):
            return low_ext[0, k + FH, PAD + j], low_ext[1, k + FH, PAD + j]

        def high(k, j):
            i = k - (n_k - FH + 1)
            return high_ext[0, i, PAD + j], high_ext[1, i, PAD + j]

        source(step, 1, local, local)
        lend(low_ext, step, FH, 0)
        lend(high_ext, step, 0, n_k - FH + 1)

        def edge(i, _):
            is_low = jnp.where(i == 0, second, first) == 0

            @pl.when(jnp.logical_and(is_low, has_down))
            def _():
                band_copy(step, 0).wait_recv()
                wrap(low_ext, 0)

            @pl.when(is_low)
            def _():
                source(step, 0, local, low)

            is_high = jnp.logical_not(is_low)

            @pl.when(jnp.logical_and(is_high, has_up))
            def _():
                band_copy(step, 1).wait_recv()
                wrap(high_ext, FH - 1)

            @pl.when(is_high)
            def _():
                source(step, groups - 1, high, local)

            return 0

        lax.fori_loop(0, 2, edge, 0)
        if step < STEPS - 1:
            send_halo(2 * step + 2, 1)

    for step in range(STEPS):
        model_step(step)

    def drain(i, _):
        slot, g = i // groups, lax.rem(i, groups)

        @pl.when(has_north)
        def _():
            row_copy(slot, 0, g).wait_send()

        @pl.when(has_south)
        def _():
            row_copy(slot, 1, g).wait_send()

        col_copy(slot, 0, g).wait_send()
        col_copy(slot, 1, g).wait_send()
        return 0

    lax.fori_loop(0, 2 * STEPS * groups, drain, 0)
    for step in range(STEPS):

        @pl.when(has_up)
        def _():
            band_copy(step, 0).wait_send()

        @pl.when(has_down)
        def _():
            band_copy(step, 1).wait_send()


def body(background, tangent, sea_mask, coupling, freq_offsets, dir_offsets):
    n_k = background.shape[0]
    groups = n_k // GROUP
    slots = 2 * STEPS
    f32 = jnp.float32
    dma = pltpu.SemaphoreType.DMA
    out = jax.ShapeDtypeStruct(background.shape, f32)
    return pl.pallas_call(
        lambda *refs: kernel(n_k, *refs),
        out_shape=(out, out),
        in_specs=[pl.BlockSpec(memory_space=pltpu.HBM)] * 6,
        out_specs=(pl.BlockSpec(memory_space=pltpu.VMEM), pl.BlockSpec(memory_space=pltpu.VMEM)),
        scratch_shapes=[
            pltpu.VMEM((2, n_k, WIDE, 8, 128), f32),
            pltpu.VMEM((2, n_k, WIDE, 8, 128), f32),
            pltpu.VMEM((2, 2 * FH - 1, WIDE, 8, 128), f32),
            pltpu.VMEM((2, 2 * FH - 1, WIDE, 8, 128), f32),
            pltpu.VMEM((2, 2 * FH - 1, WIDE, 8, 128), f32),
            pltpu.VMEM((2, 2 * FH - 1, WIDE, 8, 128), f32),
            pltpu.VMEM((slots, 2, n_k, 2, HALF, 128), f32),
            pltpu.VMEM((slots, 2, n_k, 2, HALF, 128), f32),
            pltpu.VMEM((slots, 2, groups, 8, 128), f32),
            pltpu.VMEM((slots, 2, groups, 8, 128), f32),
            pltpu.VMEM((1, 8, 128), jnp.int32),
            pltpu.SMEM((n_k,), f32),
            pltpu.SMEM((2,), jnp.int32),
            pltpu.SMEM((2,), jnp.int32),
            pltpu.SMEM((n_k,), f32),
            dma((2, groups)),
            dma((4,)),
            dma((slots, 2, groups)),
            dma((slots, 2, groups)),
            dma((slots, 2, groups)),
            dma((slots, 2, groups)),
            dma((STEPS, 2)),
            dma((STEPS, 2)),
        ],
        compiler_params=pltpu.CompilerParams(
            collective_id=0, has_side_effects=True, vmem_limit_bytes=48 * 1024 * 1024
        ),
        name="wave_steps",
    )(*[pltpu.with_memory_space_constraint(x, pltpu.HBM) for x in (background, tangent, sea_mask, coupling, freq_offsets, dir_offsets)])


def solution(mesh):
    in_specs = (
        P("band", None, "tile", None, None),
        P("band", None, "tile", None, None),
        P("tile", None, None),
        P("band"),
        P(),
        P(),
    )
    out_specs = (P("band", None, "tile", None, None), P("band", None, "tile", None, None))
    return jax.shard_map(body, mesh=mesh, in_specs=in_specs, out_specs=out_specs, check_vma=False)
```
